32 devices in a mesh: wave: 16 (over z, x, core), level: 2 (over y).
Axes of the slice: x: 2, y: 2, z: 4, core: 2. Of those that a mesh axis runs over, the one named last changes fastest.
Arguments:
- state: float32 [4, 64, 256, 2, 256], P(None, 'level', 'wave'), may hold values from -0.02 to 0.02
- legendre: float32 [256, 384, 256], P('wave'), may hold values from -6 to 6
- lat_weight: float32 [384], P('wave'), may hold values from 0.8 to 2
- modes: float32 [64, 64], replicated, may hold values from -1 to 1, as said below
- mode_rates: float32 [64], replicated, may hold values from 1e-05 to 0.003
- diffusion: float32 [4], replicated, may hold values from 0.3 to 3
- norm_gain: float32 [256], replicated, may hold values from 0.5 to 1.5
- w_first: bfloat16 [1024, 256], replicated, may hold values from -0.375 to 0.375
- b_first: float32 [1024], replicated, may hold values from -3 to 3
- w_second: bfloat16 [1024, 1024], replicated, may hold values from -0.1875 to 0.1875
- b_second: float32 [1024], replicated, may hold values from -3 to 3
- w_third: bfloat16 [256, 1024], replicated, may hold values from -0.1875 to 0.1875
- b_third: float32 [256], replicated, may hold values from -1.2 to 1.2
Outputs:
- next_state: float32 [4, 64, 256, 2, 256], P(None, 'level', 'wave')
The draws below stay inside these ranges and needn't reach their ends.
Inputs may be any that keep to these rules, and one draw needn't show every extreme that they name: `modes`: orthogonal: its transpose is its inverse.
All inputs are finite; a program needn't handle non-finite values.
Results may differ from the reference program's by a relative error of at most 0.0011.
Values may be sent and summed in bfloat16 or wider, within the bound.
A program may use at most 192 MiB of HBM per device.

```python
import math
import jax
import jax.numpy as jnp
from jax import lax

F = 4
LEV = 64
M = 256
LAT = 384
LON = 768
HID = 1024


def draw_modes(key, part):
    random_matrix = jax.random.normal(key, (LEV, LEV), jnp.float32)
    factors = jnp.linalg.qr(random_matrix)
    return factors[0].astype(jnp.float32)


def level_of(rng, extent, shards, least, largest):
    level, own = 1.0, jax.random.fold_in(rng, 6)
    for axis_at, shards_of in shards:
        heights = jnp.exp(jax.random.uniform(jax.random.fold_in(own, axis_at), (shards_of,), jnp.float32, least / len(shards), largest / len(shards)))
        level = level * jnp.repeat(heights, extent[axis_at] // shards_of).reshape([-1 if axis == axis_at else 1 for axis in range(len(extent))])
    return level


def gaussian(key, dims, deviation, bound, shards=(), kind=jnp.bfloat16):
    values = deviation * jax.random.normal(key, dims, jnp.float32)
    if shards:
        values = values * level_of(key, dims, shards, -0.22, 0.18)
    return jnp.clip(values, -bound, bound).astype(kind)


def setup_inputs(seed: int = 0) -> dict:
    key_of = jax.random.split(jax.random.key(seed), 14)
    state = gaussian(key_of[0], (F, LEV, M, 2, M), 0.003, 0.02, ((1, 2), (2, 16)), jnp.float32)
    legendre = gaussian(key_of[1], (M, LAT, M), 1.0, 6.0, ((0, 16),), jnp.float32)
    lat_weight = jnp.clip(0.8 + 1.2 * jax.random.uniform(key_of[2], (LAT,), jnp.float32) ** level_of(key_of[2], (LAT,), ((0, 16),), -0.2, 0.2), 0.8, 2.0)
    modes = draw_modes(jax.random.fold_in(key_of[13], 71), 0)
    mode_rates = jnp.clip(jnp.exp(jax.random.uniform(key_of[4], (LEV,), jnp.float32, math.log(9.999999747378752e-06), math.log(0.003))), 9.999999747378752e-06, 0.003)
    diffusion = jnp.clip(jnp.exp(jax.random.uniform(key_of[5], (F,), jnp.float32, math.log(0.3), math.log(3.0))), 0.3, 3.0)
    norm_gain = jnp.clip(1.0 + 0.1 * jax.random.normal(key_of[6], (F * LEV,), jnp.float32), 0.5, 1.5)
    w_first = gaussian(key_of[7], (HID, F * LEV), (F * LEV) ** -0.5, 0.375)
    b_first = gaussian(key_of[8], (HID,), 0.5, 3.0, (), jnp.float32)
    w_second = gaussian(key_of[9], (HID, HID), HID ** -0.5, 0.1875)
    b_second = gaussian(key_of[10], (HID,), 0.5, 3.0, (), jnp.float32)
    w_third = gaussian(key_of[11], (F * LEV, HID), HID ** -0.5, 0.1875)
    b_third = gaussian(key_of[12], (F * LEV,), 0.2, 1.2, (), jnp.float32)
    return dict(state=state, legendre=legendre, lat_weight=lat_weight, modes=modes, mode_rates=mode_rates, diffusion=diffusion, norm_gain=norm_gain, w_first=w_first, b_first=b_first, w_second=w_second, b_second=b_second, w_third=w_third, b_third=b_third)


highest = lax.Precision.HIGHEST
norm_eps = 1e-06

def phase_angles(waves, longitudes):
    wave_idx = jnp.arange(waves, dtype=jnp.int32)
    lon_idx = jnp.arange(longitudes, dtype=jnp.int32)
    phase_turns = wave_idx[:, None] * lon_idx[None, :] % longitudes
    return (2.0 * jnp.pi / longitudes * phase_turns.astype(jnp.float32), wave_idx)

def synthesis_table(waves, longitudes):
    angle_table, wave_idx = phase_angles(waves, longitudes)
    factor = jnp.where(wave_idx == 0, 1.0, 2.0).astype(jnp.float32)[:, None]
    return jnp.stack([factor * jnp.cos(angle_table), -factor * jnp.sin(angle_table)], axis=1)

def analysis_table(waves, longitudes):
    angle_table, wave_idx = phase_angles(waves, longitudes)
    flipped = angle_table.T
    return jnp.stack([jnp.cos(flipped), -jnp.sin(flipped)], axis=2) / longitudes

def column_physics(columns, norm_gain, w_first, b_first, w_second, b_second, w_third, b_third):
    values = columns.astype(jnp.float32)
    inverse_rms = lax.rsqrt(lax.optimization_barrier(jnp.mean(values * values, axis=0, keepdims=True)) + norm_eps)
    normed = (values * inverse_rms * norm_gain[:, None]).astype(jnp.bfloat16)
    hidden_one = jax.nn.gelu(jnp.dot(w_first.astype(jnp.float32), normed.astype(jnp.float32), preferred_element_type=jnp.float32) + b_first[:, None]).astype(jnp.bfloat16)
    hidden_two = jax.nn.gelu(jnp.dot(w_second.astype(jnp.float32), hidden_one.astype(jnp.float32), preferred_element_type=jnp.float32) + b_second[:, None]).astype(jnp.bfloat16)
    return (jnp.dot(w_third.astype(jnp.float32), hidden_two.astype(jnp.float32), preferred_element_type=jnp.float32) + b_third[:, None]).astype(jnp.bfloat16)

def reference(state, legendre, lat_weight, modes, mode_rates, diffusion, norm_gain, w_first, b_first, w_second, b_second, w_third, b_third):
    wave_idx = jnp.arange(M, dtype=jnp.int32)
    degree_index = wave_idx[:, None] + jnp.arange(M, dtype=jnp.int32)[None, :]
    kept_mask = (degree_index < M).astype(jnp.float32)
    kept_basis = legendre * kept_mask[:, None, :]
    band_coeffs = jnp.einsum('flmcj,maj->flmca', state, kept_basis, precision=highest)
    grid_field = jnp.einsum('flmca,mco->flao', band_coeffs, synthesis_table(M, LON), precision=highest)
    grid_low = grid_field.astype(jnp.bfloat16)

    def one_row(row_block):
        flat_cols = row_block.reshape(F * LEV, LON)
        return column_physics(flat_cols, norm_gain, w_first, b_first, w_second, b_second, w_third, b_third).reshape(F, LEV, LON)
    tendency = lax.map(one_row, jnp.moveaxis(grid_low, 2, 0))
    tendency = jnp.moveaxis(tendency, 0, 2)
    updated = (grid_field + tendency.astype(jnp.float32)) * lat_weight[None, None, :, None]
    wave_coeffs = jnp.einsum('flao,omc->flmca', updated, analysis_table(M, LON), precision=highest)
    spectral = jnp.einsum('flmca,maj->flmcj', wave_coeffs, kept_basis, precision=highest)
    growth = (degree_index * (degree_index + 1)).astype(jnp.float32)
    amplitude = jnp.einsum('lk,lmcj->kmcj', modes, spectral[1], precision=highest)
    amplitude = amplitude / (1.0 + mode_rates[:, None, None, None] * growth[None, :, None, :])
    solved = jnp.einsum('lk,kmcj->lmcj', modes, amplitude, precision=highest)
    combined = jnp.concatenate([spectral[:1], solved[None], spectral[2:]], axis=0)
    scaled_growth = growth / (M * (M - 1))
    damping = 1.0 + diffusion[:, None, None] * (scaled_growth * scaled_growth)[None]
    return combined / damping[:, None, :, None, :]
```

```python
import functools
import math

import jax
import jax.numpy as jnp
import numpy as np
from jax import lax
from jax.experimental import pallas as pl
from jax.experimental.pallas import tpu as pltpu
from jax.sharding import PartitionSpec as P

high = lax.Precision.HIGH
norm_eps = 1e-06
axes = ("wave", "level")
send_scale = 1024.0


def phase_angles(waves, longitudes):
    wave_idx = jnp.arange(waves, dtype=jnp.int32)
    lon_idx = jnp.arange(longitudes, dtype=jnp.int32)
    phase_turns = wave_idx[:, None] * lon_idx[None, :] % longitudes
    return (2.0 * jnp.pi / longitudes * phase_turns.astype(jnp.float32), wave_idx)


def synthesis_table(waves, longitudes):
    angle_table, wave_idx = phase_angles(waves, longitudes)
    factor = jnp.where(wave_idx == 0, 1.0, 2.0).astype(jnp.float32)[:, None]
    return jnp.stack([factor * jnp.cos(angle_table), -factor * jnp.sin(angle_table)], axis=1)


def analysis_table(waves, longitudes):
    angle_table, _ = phase_angles(waves, longitudes)
    return jnp.stack([jnp.cos(angle_table), -jnp.sin(angle_table)], axis=1) / longitudes


def contract_last(left, right):
    return lax.dot_general(
        left, right, (((1,), (1,)), ((), ())), preferred_element_type=jnp.float32
    )


def physics_kernel(grid_ref, lat_ref, gain_ref, w1_ref, b1_ref, w2_ref, b2_ref, w3_ref, b3_ref, out_ref, top_ref):
    grid_rows = grid_ref[0]
    values = grid_rows.astype(jnp.bfloat16).astype(jnp.float32)
    inverse_rms = lax.rsqrt(jnp.mean(values * values, axis=1, keepdims=True) + norm_eps)
    normed = (values * inverse_rms * gain_ref[...]).astype(jnp.bfloat16)
    hidden = jax.nn.gelu(contract_last(normed, w1_ref[...]) + b1_ref[...]).astype(jnp.bfloat16)
    hidden = jax.nn.gelu(contract_last(hidden, w2_ref[...]) + b2_ref[...]).astype(jnp.bfloat16)
    tendency = (contract_last(hidden, w3_ref[...]) + b3_ref[...]).astype(jnp.bfloat16)
    updated = (grid_rows + tendency.astype(jnp.float32)) * lat_ref[pl.program_id(0)]
    out_ref[0] = updated
    top_ref[0] = jnp.max(jnp.abs(updated), axis=0, keepdims=True)


def column_step(grid, lat, gain, w1, b1, w2, b2, w3, b3):
    rows, lon, feats = grid.shape
    hid = w1.shape[0]
    whole = lambda *shape: pl.BlockSpec(shape, lambda i: (0,) * len(shape))
    block = pl.BlockSpec((1, lon, feats), lambda i: (i, 0, 0))
    return pl.pallas_call(
        physics_kernel,
        grid=(rows,),
        out_shape=(
            jax.ShapeDtypeStruct((rows, lon, feats), jnp.float32),
            jax.ShapeDtypeStruct((rows, 1, feats), jnp.float32),
        ),
        in_specs=[
            block,
            pl.BlockSpec(memory_space=pltpu.SMEM),
            whole(1, feats),
            whole(hid, feats),
            whole(1, hid),
            whole(hid, hid),
            whole(1, hid),
            whole(feats, hid),
            whole(1, feats),
        ],
        out_specs=(block, pl.BlockSpec((1, 1, feats), lambda i: (i, 0, 0))),
        compiler_params=pltpu.CompilerParams(vmem_limit_bytes=56 * 1024 * 1024),
    )(grid, lat, gain[None], w1, b1[None], w2, b2[None], w3, b3[None])


def general_body(
    longitudes,
    state,
    legendre,
    lat_weight,
    modes,
    mode_rates,
    diffusion,
    norm_gain,
    w_first,
    b_first,
    w_second,
    b_second,
    w_third,
    b_third,
):
    fields, lev_dev, m_dev, parts, degrees = state.shape
    levels = modes.shape[0]
    waves = degrees
    wave_count = lax.axis_size("wave")
    level_count = lax.axis_size("level")
    lat_band = lat_weight.shape[0]
    lat_own = -(-lat_band // level_count)
    lat_extra = lat_own * level_count - lat_band
    wave_global = lax.axis_index("wave") * m_dev + jnp.arange(m_dev, dtype=jnp.int32)
    degree_index = wave_global[:, None] + jnp.arange(degrees, dtype=jnp.int32)[None, :]
    kept_mask = (degree_index < waves).astype(jnp.float32)
    basis = legendre * kept_mask[:, None, :]
    if lat_extra:
        basis = basis.reshape(m_dev, wave_count, lat_band, degrees)
        basis = jnp.pad(basis, ((0, 0), (0, 0), (0, lat_extra), (0, 0)))
        basis = basis.reshape(m_dev, -1, degrees)
        lat_weight = jnp.pad(lat_weight, (0, lat_extra))
    inverse_tab = synthesis_table(waves, longitudes).reshape(wave_count, m_dev, parts, longitudes)
    forward_tab = analysis_table(waves, longitudes).reshape(wave_count, m_dev, parts, longitudes)

    band = jnp.einsum("flmcj,maj->amcfl", state, basis, precision=high)
    band = (band * send_scale).astype(jnp.float16)
    band = band.reshape(wave_count * level_count, lat_own, m_dev, parts, fields, lev_dev)
    band = lax.all_to_all(band, axes, split_axis=0, concat_axis=0, tiled=True)
    band = band.reshape(wave_count, level_count, lat_own, m_dev, parts, fields, lev_dev)
    band = band.astype(jnp.float32) * (1.0 / send_scale)
    grid = jnp.einsum("wvamcfl,wmco->aovfl", band, inverse_tab, precision=high)
    feats = fields * levels
    grid = grid.reshape(lat_own, longitudes, feats)

    def slabs_first(x):
        split = x.reshape((fields, level_count, lev_dev) + x.shape[1:])
        return jnp.swapaxes(split, 0, 1).reshape(x.shape)

    lat = lax.dynamic_slice_in_dim(lat_weight, lax.axis_index("level") * lat_own, lat_own, 0)
    updated, tops = column_step(
        grid,
        lat,
        slabs_first(norm_gain),
        slabs_first(w_first.T).T,
        b_first,
        w_second,
        b_second,
        slabs_first(w_third),
        slabs_first(b_third),
    )
    top = jnp.maximum(jnp.max(tops), 1e-25)
    reach = 32768.0 / levels**0.5
    tops_all = lax.all_gather(top / reach, axes).reshape(wave_count, level_count)

    wave = jnp.einsum("aok,wmco->wmcak", updated, forward_tab, precision=high)
    wave = wave * (reach / top)
    wave = wave.reshape(wave_count, m_dev, parts, lat_own, level_count, fields, lev_dev)
    modal = jnp.einsum(
        "wmcavl,vlk->wmcak",
        wave[..., 1, :],
        modes.reshape(level_count, lev_dev, levels),
        precision=high,
    )
    others = jnp.concatenate([wave[..., :1, :], wave[..., 2:, :]], axis=-2)
    others = others.reshape(wave_count, m_dev, parts, lat_own, level_count, (fields - 1) * lev_dev)
    others = jnp.moveaxis(others, 4, 1)
    modal = jnp.broadcast_to(modal[:, None], others.shape[:-1] + (levels,))
    sent = jnp.concatenate([others, modal], axis=-1).astype(jnp.float16)
    sent = sent.reshape((wave_count * level_count,) + sent.shape[2:])
    got = lax.all_to_all(sent, axes, split_axis=0, concat_axis=0, tiled=True)
    got = got.reshape((wave_count, level_count) + got.shape[1:]).astype(jnp.float32)
    got = got * tops_all[:, :, None, None, None, None]
    basis_split = basis.reshape(m_dev, wave_count, level_count, lat_own, degrees)
    spectral = jnp.einsum("wvmcaq,mwvaj->qmcj", got, basis_split, precision=high)

    growth = (degree_index * (degree_index + 1)).astype(jnp.float32)
    plain = spectral[: (fields - 1) * lev_dev].reshape(fields - 1, lev_dev, m_dev, parts, degrees)
    divisor = 1.0 + mode_rates[:, None, None, None] * growth[None, :, None, :]
    amplitude = spectral[(fields - 1) * lev_dev :] / divisor
    own_rows = lax.dynamic_slice_in_dim(modes, lax.axis_index("level") * lev_dev, lev_dev, 0)
    solved = jnp.einsum("lk,kmcj->lmcj", own_rows, amplitude, precision=high)
    combined = jnp.concatenate([plain[:1], solved[None], plain[1:]], axis=0)
    scaled_growth = growth / (waves * (waves - 1))
    damping = 1.0 + diffusion[:, None, None] * (scaled_growth * scaled_growth)[None]
    return combined / damping[:, None, :, None, :]


chunks = 3
vmem_limit = 60 * 1024 * 1024


def split_table(table):
    high_part = np.asarray(table, jnp.bfloat16)
    low_part = np.asarray(table - high_part.astype(np.float64), jnp.bfloat16)
    return np.stack([high_part, low_part])


def fourier_tables(waves, longitudes, wave_count, scale):
    half = longitudes // 2
    per_wave = waves // wave_count
    synthesis, analysis = [], []
    for parity in range(2):
        order = np.arange(waves).reshape(wave_count, per_wave // 2, 2)[:, :, parity]
        turns = order[:, :, None] * np.arange(half)[None, None, :] % longitudes
        angles = 2.0 * np.pi / longitudes * turns
        pair = np.stack([np.cos(angles), -np.sin(angles)], axis=1)
        factor = np.where(order == 0, 1.0, 2.0)[:, None, :, None]
        synthesis.append(split_table((pair * factor / scale).reshape(-1, half).T))
        analysis.append(split_table((pair / longitudes).reshape(-1, half)))
    return np.stack(synthesis), np.stack(analysis)


def halves(x):
    top = x.astype(jnp.bfloat16)
    return top, (x - top.astype(jnp.float32)).astype(jnp.bfloat16)


def dot3(left, right, dims):
    dot = lambda a, b: lax.dot_general(a, b, (dims, ((), ())), preferred_element_type=jnp.float32)
    return dot(left[0], right[0]) + (dot(left[0], right[1]) + dot(left[1], right[0]))


def kept(block, wave_index):
    degree = lax.broadcasted_iota(jnp.int32, block.shape, 1)
    return jnp.where(degree + wave_index < block.shape[1], block, 0.0)


def row_of(m, part, m_dev):
    half = m_dev // 2
    return (m % 2) * m_dev + part * half + m // 2


send_octaves, send_top = 32, 5
back_octaves, back_top = 56, 24


def encode(x, octaves, top):
    floor_power = float(top - octaves)
    magnitude = jnp.abs(x)
    power = jnp.floor(jnp.log2(jnp.maximum(magnitude, 2.0**floor_power)))
    ratio = 250.0 / (octaves + 1)
    place = (magnitude * jnp.exp2(-power) + (power - floor_power)) * ratio
    step = jnp.floor(place)
    code = jnp.exp2(step - 125.0) * (place - step + 1.0)
    return jnp.where(x < 0.0, -code, code).astype(jnp.bfloat16)


def decode(code, octaves, top):
    floor_power = float(top - octaves)
    code = code.astype(jnp.float32)
    magnitude = jnp.abs(code)
    step = jnp.floor(jnp.log2(magnitude))
    place = (magnitude * jnp.exp2(-step) + (step + 124.0)) * ((octaves + 1) / 250.0)
    power = jnp.floor(place)
    lead = jnp.minimum(power, 1.0)
    value = (place - power + lead) * jnp.exp2(power - lead + floor_power)
    return jnp.where(code < 0.0, -value, value)


def own_place():
    slabs = lax.axis_size("level")
    count = lax.axis_size("wave") * slabs
    return lax.axis_index("wave") * slabs + lax.axis_index("level"), count, slabs


def start_wave(src, dst, sems, at):
    me, count, slabs = own_place()
    half = count // 2
    side = me // half

    def to(base, first):
        peer = base * half + lax.rem(me + first, half)
        pltpu.make_async_remote_copy(
            src_ref=src.at[at, peer],
            dst_ref=dst.at[at, me],
            send_sem=sems.at[0, at],
            recv_sem=sems.at[1, at],
            device_id=(peer // slabs, lax.rem(peer, slabs)),
            device_id_type=pl.DeviceIdType.MESH,
        ).start()
        return 0

    lax.fori_loop(0, half, lambda k, _: to(1 - side, k), 0)
    lax.fori_loop(1, half, lambda k, _: to(side, k), 0)


def wait_most(src, dst, sem, at, count):
    most = pl.ds(0, count - 1)
    pltpu.make_async_copy(src.at[at, most], dst.at[at, most], sem).wait()


def whole_block(x):
    return pl.BlockSpec(x.shape, lambda *_: (0,) * x.ndim)


def remote_params():
    return pltpu.CompilerParams(vmem_limit_bytes=vmem_limit, has_side_effects=True)


def twice_gelu(x):
    inner = x * (0.7978845608028654 + 0.7978845608028654 * 0.044715 * (x * x))
    return (x + x * jnp.tanh(inner)).astype(jnp.bfloat16)


def step_kernel(
    lat_ref, diff_ref, state_ref, leg_ref, modes_ref, rates_ref, gain_ref, b1_ref, b2_ref, b3_ref, perm_ref, syn_hbm, ana_hbm, w1_hbm, w2_hbm, w3_hbm,
    out_ref, swap_ref,
    band_ref, there_ref, here_ref, back_ref, home_ref, total_ref, hold_ref, modal_ref, gain_own, b3_own, syn_ref, ana_ref, w1_ref, w2_ref, w3_ref,
    there_sems, back_sems, swap_sems, load_sems,
):
    fields, lev_dev, m_block, parts, degrees = state_ref.shape
    rows = back_ref.shape[0]
    step = pl.program_id(0)
    first_steps = (pl.num_programs(0) - rows) // 2
    blocks = first_steps // chunks
    grid_steps = first_steps + rows
    m_dev = blocks * m_block
    feats = fields * lev_dev
    mc = m_dev * parts
    half = mc // 2
    me, count, slabs = own_place()
    waves = count // slabs
    width = slabs * feats
    per_chunk = rows // chunks
    level = lax.axis_index("level")
    loads = [
        pltpu.make_async_copy(src, dst, load_sems.at[i])
        for i, (src, dst) in enumerate(((syn_hbm, syn_ref), (ana_hbm, ana_ref), (w1_hbm, w1_ref), (w2_hbm, w2_ref), (w3_hbm, w3_ref)))
    ]

    @pl.when(step == 0)
    def _():
        for load in loads:
            load.start()

    @pl.when((step > 0) & (step <= first_steps) & (lax.rem(step, blocks) == 0))
    def _():
        start_wave(there_ref, here_ref, there_sems, step // blocks - 1)

    @pl.when(step == blocks)
    def _():
        for load in loads:
            load.wait()
        order = [slice((f * slabs + v) * lev_dev, (f * slabs + v + 1) * lev_dev) for v in range(slabs) for f in range(fields)]
        gain_own[...] = jnp.concatenate([gain_ref[:, at] for at in order], axis=1)
        b3_own[...] = jnp.concatenate([b3_ref[:, at] for at in order], axis=1)
        w3_ref[...] = jnp.concatenate([w3_ref[at, :] for at in order], axis=0) * 0.5
        w1_ref[...] = jnp.dot(w1_ref[...], perm_ref[...], preferred_element_type=jnp.float32).astype(jnp.bfloat16)
        w2_ref[...] = w2_ref[...] * 0.5
        same = lax.broadcasted_iota(jnp.int32, (width, width), 0) == lax.broadcasted_iota(jnp.int32, (width, width), 1)
        modal_ref[...] = same.astype(jnp.float32)
        total_ref[...] = jnp.zeros_like(total_ref)
        for v in range(slabs):
            for k in range(slabs):
                at = lambda i: slice(i * feats + lev_dev, i * feats + 2 * lev_dev)
                modal_ref[at(v), at(k)] = modes_ref[v * lev_dev : (v + 1) * lev_dev, k * lev_dev : (k + 1) * lev_dev]

    @pl.when(step < first_steps)
    def _():
        group, block = step // blocks, lax.rem(step, blocks)
        for i in range(m_block):
            m = block * m_block + i
            basis = leg_ref[i].reshape(-1, degrees)
            basis = halves(kept(basis, lax.axis_index("wave") * m_dev + m))
            coeffs = [state_ref[:, :, i, c, :].reshape(feats, degrees) for c in range(parts)]
            coeffs = halves(jnp.concatenate(coeffs, axis=0))
            band = dot3(basis, coeffs, ((1,), (1,)))
            for c in range(parts):
                at = pl.ds(row_of(m, c, m_dev), band.shape[0], stride=mc)
                band_ref[at, :] = band[:, c * feats : (c + 1) * feats]

        @pl.when(block == blocks - 1)
        def _():
            size = per_chunk * mc
            many = 4

            def one(k, _):
                part = band_ref[pl.ds(pl.multiple_of(k * many * size, 8), many * size), :]
                there_ref[group, pl.ds(k * many, many)] = encode(part, send_octaves, send_top).reshape(many, size, feats)
                return 0

            lax.fori_loop(0, count // many, one, 0)
            here_ref[group, me] = there_ref[group, me]

    @pl.when((step > first_steps) & (step <= grid_steps))
    def _():
        start_wave(back_ref, home_ref, back_sems, step - first_steps - 1)

    @pl.when((step >= first_steps) & (step < grid_steps))
    def _():
        row = step - first_steps
        group, place = row // per_chunk, lax.rem(row, per_chunk)

        @pl.when(place == 0)
        def _():
            wait_most(there_ref, here_ref, there_sems.at[1, group], group, count)

        signs = []
        for parity in range(2):
            at = pl.ds(pl.multiple_of(place * mc + parity * half, half), half)
            band = decode(here_ref[group, :, at, :], send_octaves, send_top).reshape(waves, slabs, half, feats)
            band = [band[:, v].reshape(waves * half, feats) for v in range(slabs)]
            band = halves(jnp.concatenate(band, axis=1))
            signs.append(dot3((syn_ref[parity, 0], syn_ref[parity, 1]), band, ((1,), (0,))))
        weight = lat_ref[group * (slabs * per_chunk) + level * per_chunk + place]
        updated = []
        for grid in (signs[0] + signs[1], signs[0] - signs[1]):
            values = grid.astype(jnp.bfloat16).astype(jnp.float32)
            inverse_rms = lax.rsqrt(jnp.mean(values * values, axis=1, keepdims=True) + norm_eps)
            normed = (values * inverse_rms * gain_own[...]).astype(jnp.bfloat16)
            hidden = twice_gelu(contract_last(normed, w1_ref[...]) + b1_ref[...])
            hidden = twice_gelu(contract_last(hidden, w2_ref[...]) + b2_ref[...])
            tendency = (contract_last(hidden, w3_ref[...]) + b3_own[...]).astype(jnp.bfloat16)
            updated.append((grid + tendency.astype(jnp.float32)) * weight)
        folded = (updated[0] + updated[1], updated[0] - updated[1])
        modal = halves(modal_ref[...])
        lane = lax.broadcasted_iota(jnp.int32, (waves, half // 2, feats), 2)
        swapped = (lane >= lev_dev) & (lane < 2 * lev_dev)
        for parity in range(2):
            wave = dot3((ana_ref[parity, 0], ana_ref[parity, 1]), halves(folded[parity]), ((1,), (0,)))
            wave = dot3(halves(wave), modal, ((1,), (0,)))
            piece = lambda c, v: wave[:, v * feats : (v + 1) * feats].reshape(waves, 2, half // 2, feats)[:, c]
            for v in range(slabs):
                both = [jnp.where(swapped, piece(v, c), piece(c, v)) for c in range(2)]
                both = encode(jnp.concatenate(both, axis=1), back_octaves, back_top)
                for w in range(waves):
                    back_ref[row, w * slabs + v, parity * half : (parity + 1) * half, :] = both[w]

        home_ref[row, me] = back_ref[row, me]

    late = step - grid_steps
    late_group, late_block = late // blocks, lax.rem(late, blocks)

    @pl.when((step >= grid_steps) & (late_block == 0))
    def _():
        wave_ref = band_ref.reshape(count, per_chunk, mc, feats)

        def one(r, _):
            row = late_group * per_chunk + r
            wait_most(back_ref, home_ref, back_sems.at[1, row], row, count)
            wave_ref[:, r] = decode(home_ref[row], back_octaves, back_top)
            return 0

        lax.fori_loop(0, per_chunk, one, 0)

    def analysed(i):
        m = late_block * m_block + i
        basis = leg_ref[i].reshape(-1, degrees)
        basis = halves(kept(basis, lax.axis_index("wave") * m_dev + m))
        wave = [band_ref[pl.ds(row_of(m, c, m_dev), basis[0].shape[0], stride=mc), :] for c in range(parts)]
        return m, dot3(halves(jnp.concatenate(wave, axis=1)), basis, ((0,), (0,)))

    @pl.when((step >= grid_steps) & (late_group < chunks - 1))
    def _():
        for i in range(m_block):
            m, part = analysed(i)
            total_ref[m] = total_ref[m] + part

    def swap(at):
        return pltpu.make_async_remote_copy(
            src_ref=hold_ref.at[at],
            dst_ref=swap_ref.at[at],
            send_sem=swap_sems.at[0, at],
            recv_sem=swap_sems.at[1, at],
            device_id=(lax.axis_index("wave"), 1 - level),
            device_id_type=pl.DeviceIdType.MESH,
        )

    @pl.when((step >= grid_steps) & (late_group == chunks - 1))
    def _():
        @pl.when(late_block > 0)
        def _():
            swap(late_block - 1).start()

        own = halves(modes_ref[pl.ds(pl.multiple_of(level * lev_dev, 8), lev_dev), :])
        other = halves(modes_ref[pl.ds(pl.multiple_of((1 - level) * lev_dev, 8), lev_dev), :])
        for i in range(m_block):
            m, part = analysed(i)
            spectral = total_ref[m] + part
            degree = lax.axis_index("wave") * m_dev + m + lax.broadcasted_iota(jnp.int32, (1, degrees), 1)
            growth = (degree * (degree + 1)).astype(jnp.float32)
            scaled_growth = growth / (degrees * (degrees - 1))
            square = scaled_growth * scaled_growth
            for f in range(fields):
                if f != 1:
                    inverse = 1.0 / (1.0 + diff_ref[f] * square)
                    for c in range(parts):
                        first = c * feats + f * lev_dev
                        out_ref[f, :, i, c, :] = spectral[first : first + lev_dev] * inverse
            modal = [spectral[c * feats + lev_dev : c * feats + 2 * lev_dev] for c in range(parts)]
            rates = lax.dot_general(
                rates_ref[...], growth, (((0,), (0,)), ((), ())), precision=lax.Precision.HIGHEST, preferred_element_type=jnp.float32
            )
            amplitude = halves(jnp.concatenate(modal, axis=0) / (1.0 + rates))
            inverse = 1.0 / (1.0 + diff_ref[1] * square)
            mine = dot3(own, amplitude, ((1,), (0,))) * inverse
            for c in range(parts):
                out_ref[1, :, i, c, :] = mine
            hold_ref[late_block, i] = encode(dot3(other, amplitude, ((1,), (0,))) * inverse, back_octaves, back_top)

    @pl.when(step == pl.num_programs(0) - 1)
    def _():
        swap(blocks - 1).start()
        lax.fori_loop(0, chunks, lambda at, _: (wait_most(there_ref, here_ref, there_sems.at[0, at], at, count), 0)[1], 0)
        lax.fori_loop(0, rows, lambda at, _: (wait_most(back_ref, home_ref, back_sems.at[0, at], at, count), 0)[1], 0)
        lax.fori_loop(0, blocks, lambda at, _: (swap(at).wait(), 0)[1], 0)


def whole_step(state, legendre, lat, diffusion, modes, rates, gain, b1, b2, b3, perm, synthesis, analysis, w1, w2, w3):
    fields, lev_dev, m_dev, parts, degrees = state.shape
    waves, slabs = lax.axis_size("wave"), lax.axis_size("level")
    count, feats, mc = waves * slabs, fields * lev_dev, m_dev * parts
    tile = legendre.shape[1] // (waves * chunks)
    legendre = legendre.reshape(m_dev, waves, chunks, tile, degrees)
    per_chunk = tile // slabs
    rows = chunks * per_chunk
    m_block = 4
    blocks = m_dev // m_block
    first_steps = chunks * blocks
    last = first_steps - 1
    grid_steps = first_steps + rows
    there = (chunks, count, per_chunk * mc, feats)
    back = (rows, count, mc, feats)
    small = (modes, rates, gain, b1, b2, b3, perm)
    large = (synthesis, analysis, w1, w2, w3)
    swap = (blocks, m_block, lev_dev, degrees)
    any_spec = pl.BlockSpec(memory_space=pl.ANY)
    smem = pl.BlockSpec(memory_space=pltpu.SMEM)
    bf16, f32 = jnp.bfloat16, jnp.float32
    pair = lambda i: jnp.where(i < first_steps, i, jnp.maximum(i - grid_steps, 0))
    return pl.pallas_call(
        step_kernel,
        grid=(grid_steps + first_steps,),
        out_shape=(jax.ShapeDtypeStruct(state.shape, f32), jax.ShapeDtypeStruct(swap, bf16)),
        in_specs=[
            smem,
            smem,
            pl.BlockSpec((fields, lev_dev, m_block, parts, degrees), lambda i: (0, 0, jnp.minimum(i, last) % blocks, 0, 0)),
            pl.BlockSpec((m_block, waves, None, tile, degrees), lambda i: (pair(i) % blocks, 0, pair(i) // blocks, 0, 0)),
            *[whole_block(x) for x in small],
            *[any_spec for _ in large],
        ],
        out_specs=(
            pl.BlockSpec((fields, lev_dev, m_block, parts, degrees), lambda i: (0, 0, jnp.maximum(i - (grid_steps + first_steps - blocks), 0), 0, 0)),
            any_spec,
        ),
        scratch_shapes=[
            pltpu.VMEM((count * per_chunk * mc, feats), f32),
            pltpu.VMEM(there, bf16),
            pltpu.VMEM(there, bf16),
            pltpu.VMEM(back, bf16),
            pltpu.VMEM(back, bf16),
            pltpu.VMEM((m_dev, parts * feats, degrees), f32),
            pltpu.VMEM(swap, bf16),
            pltpu.VMEM((slabs * feats, slabs * feats), f32),
            pltpu.VMEM(gain.shape, f32),
            pltpu.VMEM(b3.shape, f32),
            *[pltpu.VMEM(x.shape, bf16) for x in large],
            pltpu.SemaphoreType.DMA((2, chunks)),
            pltpu.SemaphoreType.DMA((2, rows)),
            pltpu.SemaphoreType.DMA((2, blocks)),
            pltpu.SemaphoreType.DMA((len(large),)),
        ],
        compiler_params=remote_params(),
    )(lat, diffusion, state, legendre, *small, *large)


def merge_kernel(old_ref, got_ref, out_ref):
    level = lax.axis_index("level")
    got = jnp.swapaxes(decode(got_ref[0], back_octaves, back_top), 0, 1)
    for f in range(out_ref.shape[0]):
        if f != 1:
            out_ref[f] = old_ref[f]
    for c in range(2):
        out_ref[1, :, :, c, :] = jnp.where(level == c, old_ref[1, :, :, c, :], got)


def merge_step(state, got):
    fields, lev_dev, m_dev, parts, degrees = state.shape
    blocks, m_block = got.shape[:2]
    block = pl.BlockSpec((fields, lev_dev, m_block, parts, degrees), lambda i: (0, 0, i, 0, 0))
    return pl.pallas_call(
        merge_kernel,
        grid=(blocks,),
        out_shape=jax.ShapeDtypeStruct(state.shape, jnp.float32),
        in_specs=[block, pl.BlockSpec((1, m_block, lev_dev, degrees), lambda i: (i, 0, 0, 0))],
        out_specs=block,
    )(state, got)


def fast_body(longitudes, state, legendre, lat_weight, modes, mode_rates, diffusion, norm_gain, w_first, b_first, w_second, b_second, w_third, b_third):
    fields, lev_dev, m_dev, parts, degrees = state.shape
    levels = modes.shape[0]
    wave_count, level_count = lax.axis_size("wave"), lax.axis_size("level")
    synthesis, analysis = fourier_tables(degrees, longitudes, wave_count, 1.0)
    place = np.arange(fields * levels).reshape(fields, level_count, lev_dev).swapaxes(0, 1).reshape(-1)
    perm = np.zeros((fields * levels, fields * levels), jnp.bfloat16)
    perm[place, np.arange(fields * levels)] = 1.0
    out, got = whole_step(
        state,
        legendre,
        lat_weight,
        diffusion,
        modes,
        mode_rates[None],
        norm_gain[None],
        b_first[None],
        b_second[None],
        b_third[None],
        perm,
        synthesis,
        analysis,
        w_first,
        w_second,
        w_third,
    )
    return merge_step(out, got)


def solution(mesh):
    wave_count, level_count = mesh.shape["wave"], mesh.shape["level"]

    def step(state, legendre, *rest):
        longitudes = 2 * legendre.shape[1]
        fields, levels, waves, _, degrees = state.shape
        fits = (
            level_count == 2
            and waves % (16 * wave_count) == 0
            and fields * levels % (128 * level_count) == 0
            and levels % (8 * level_count) == 0
            and legendre.shape[1] % (8 * chunks * wave_count) == 0
            and degrees % 128 == 0
        )
        mapped = jax.shard_map(
            functools.partial(fast_body if fits else general_body, longitudes),
            mesh=mesh,
            in_specs=(P(None, "level", "wave", None, None), P("wave", None, None), P("wave")) + (P(),) * 10,
            out_specs=P(None, "level", "wave", None, None),
            check_vma=False,
        )
        return mapped(state, legendre, *rest)

    return step
```

```python
import functools
import math

import jax
import jax.numpy as jnp
import numpy as np
from jax import lax
from jax.experimental import pallas as pl
from jax.experimental.pallas import tpu as pltpu
from jax.sharding import PartitionSpec as P

high = lax.Precision.HIGH
norm_eps = 1e-06
axes = ("wave", "level")
send_scale = 1024.0


def phase_angles(waves, longitudes):
    wave_idx = jnp.arange(waves, dtype=jnp.int32)
    lon_idx = jnp.arange(longitudes, dtype=jnp.int32)
    phase_turns = wave_idx[:, None] * lon_idx[None, :] % longitudes
    return (2.0 * jnp.pi / longitudes * phase_turns.astype(jnp.float32), wave_idx)


def synthesis_table(waves, longitudes):
    angle_table, wave_idx = phase_angles(waves, longitudes)
    factor = jnp.where(wave_idx == 0, 1.0, 2.0).astype(jnp.float32)[:, None]
    return jnp.stack([factor * jnp.cos(angle_table), -factor * jnp.sin(angle_table)], axis=1)


def analysis_table(waves, longitudes):
    angle_table, _ = phase_angles(waves, longitudes)
    return jnp.stack([jnp.cos(angle_table), -jnp.sin(angle_table)], axis=1) / longitudes


def contract_last(left, right):
    return lax.dot_general(
        left, right, (((1,), (1,)), ((), ())), preferred_element_type=jnp.float32
    )


def physics_kernel(grid_ref, lat_ref, gain_ref, w1_ref, b1_ref, w2_ref, b2_ref, w3_ref, b3_ref, out_ref, top_ref):
    grid_rows = grid_ref[0]
    values = grid_rows.astype(jnp.bfloat16).astype(jnp.float32)
    inverse_rms = lax.rsqrt(jnp.mean(values * values, axis=1, keepdims=True) + norm_eps)
    normed = (values * inverse_rms * gain_ref[...]).astype(jnp.bfloat16)
    hidden = jax.nn.gelu(contract_last(normed, w1_ref[...]) + b1_ref[...]).astype(jnp.bfloat16)
    hidden = jax.nn.gelu(contract_last(hidden, w2_ref[...]) + b2_ref[...]).astype(jnp.bfloat16)
    tendency = (contract_last(hidden, w3_ref[...]) + b3_ref[...]).astype(jnp.bfloat16)
    updated = (grid_rows + tendency.astype(jnp.float32)) * lat_ref[pl.program_id(0)]
    out_ref[0] = updated
    top_ref[0] = jnp.max(jnp.abs(updated), axis=0, keepdims=True)


def column_step(grid, lat, gain, w1, b1, w2, b2, w3, b3):
    rows, lon, feats = grid.shape
    hid = w1.shape[0]
    whole = lambda *shape: pl.BlockSpec(shape, lambda i: (0,) * len(shape))
    block = pl.BlockSpec((1, lon, feats), lambda i: (i, 0, 0))
    return pl.pallas_call(
        physics_kernel,
        grid=(rows,),
        out_shape=(
            jax.ShapeDtypeStruct((rows, lon, feats), jnp.float32),
            jax.ShapeDtypeStruct((rows, 1, feats), jnp.float32),
        ),
        in_specs=[
            block,
            pl.BlockSpec(memory_space=pltpu.SMEM),
            whole(1, feats),
            whole(hid, feats),
            whole(1, hid),
            whole(hid, hid),
            whole(1, hid),
            whole(feats, hid),
            whole(1, feats),
        ],
        out_specs=(block, pl.BlockSpec((1, 1, feats), lambda i: (i, 0, 0))),
        compiler_params=pltpu.CompilerParams(vmem_limit_bytes=56 * 1024 * 1024),
    )(grid, lat, gain[None], w1, b1[None], w2, b2[None], w3, b3[None])


def general_body(
    longitudes,
    state,
    legendre,
    lat_weight,
    modes,
    mode_rates,
    diffusion,
    norm_gain,
    w_first,
    b_first,
    w_second,
    b_second,
    w_third,
    b_third,
):
    fields, lev_dev, m_dev, parts, degrees = state.shape
    levels = modes.shape[0]
    waves = degrees
    wave_count = lax.axis_size("wave")
    level_count = lax.axis_size("level")
    lat_band = lat_weight.shape[0]
    lat_own = -(-lat_band // level_count)
    lat_extra = lat_own * level_count - lat_band
    wave_global = lax.axis_index("wave") * m_dev + jnp.arange(m_dev, dtype=jnp.int32)
    degree_index = wave_global[:, None] + jnp.arange(degrees, dtype=jnp.int32)[None, :]
    kept_mask = (degree_index < waves).astype(jnp.float32)
    basis = legendre * kept_mask[:, None, :]
    if lat_extra:
        basis = basis.reshape(m_dev, wave_count, lat_band, degrees)
        basis = jnp.pad(basis, ((0, 0), (0, 0), (0, lat_extra), (0, 0)))
        basis = basis.reshape(m_dev, -1, degrees)
        lat_weight = jnp.pad(lat_weight, (0, lat_extra))
    inverse_tab = synthesis_table(waves, longitudes).reshape(wave_count, m_dev, parts, longitudes)
    forward_tab = analysis_table(waves, longitudes).reshape(wave_count, m_dev, parts, longitudes)

    band = jnp.einsum("flmcj,maj->amcfl", state, basis, precision=high)
    band = (band * send_scale).astype(jnp.float16)
    band = band.reshape(wave_count * level_count, lat_own, m_dev, parts, fields, lev_dev)
    band = lax.all_to_all(band, axes, split_axis=0, concat_axis=0, tiled=True)
    band = band.reshape(wave_count, level_count, lat_own, m_dev, parts, fields, lev_dev)
    band = band.astype(jnp.float32) * (1.0 / send_scale)
    grid = jnp.einsum("wvamcfl,wmco->aovfl", band, inverse_tab, precision=high)
    feats = fields * levels
    grid = grid.reshape(lat_own, longitudes, feats)

    def slabs_first(x):
        split = x.reshape((fields, level_count, lev_dev) + x.shape[1:])
        return jnp.swapaxes(split, 0, 1).reshape(x.shape)

    lat = lax.dynamic_slice_in_dim(lat_weight, lax.axis_index("level") * lat_own, lat_own, 0)
    updated, tops = column_step(
        grid,
        lat,
        slabs_first(norm_gain),
        slabs_first(w_first.T).T,
        b_first,
        w_second,
        b_second,
        slabs_first(w_third),
        slabs_first(b_third),
    )
    top = jnp.maximum(jnp.max(tops), 1e-25)
    reach = 32768.0 / levels**0.5
    tops_all = lax.all_gather(top / reach, axes).reshape(wave_count, level_count)

    wave = jnp.einsum("aok,wmco->wmcak", updated, forward_tab, precision=high)
    wave = wave * (reach / top)
    wave = wave.reshape(wave_count, m_dev, parts, lat_own, level_count, fields, lev_dev)
    modal = jnp.einsum(
        "wmcavl,vlk->wmcak",
        wave[..., 1, :],
        modes.reshape(level_count, lev_dev, levels),
        precision=high,
    )
    others = jnp.concatenate([wave[..., :1, :], wave[..., 2:, :]], axis=-2)
    others = others.reshape(wave_count, m_dev, parts, lat_own, level_count, (fields - 1) * lev_dev)
    others = jnp.moveaxis(others, 4, 1)
    modal = jnp.broadcast_to(modal[:, None], others.shape[:-1] + (levels,))
    sent = jnp.concatenate([others, modal], axis=-1).astype(jnp.float16)
    sent = sent.reshape((wave_count * level_count,) + sent.shape[2:])
    got = lax.all_to_all(sent, axes, split_axis=0, concat_axis=0, tiled=True)
    got = got.reshape((wave_count, level_count) + got.shape[1:]).astype(jnp.float32)
    got = got * tops_all[:, :, None, None, None, None]
    basis_split = basis.reshape(m_dev, wave_count, level_count, lat_own, degrees)
    spectral = jnp.einsum("wvmcaq,mwvaj->qmcj", got, basis_split, precision=high)

    growth = (degree_index * (degree_index + 1)).astype(jnp.float32)
    plain = spectral[: (fields - 1) * lev_dev].reshape(fields - 1, lev_dev, m_dev, parts, degrees)
    divisor = 1.0 + mode_rates[:, None, None, None] * growth[None, :, None, :]
    amplitude = spectral[(fields - 1) * lev_dev :] / divisor
    own_rows = lax.dynamic_slice_in_dim(modes, lax.axis_index("level") * lev_dev, lev_dev, 0)
    solved = jnp.einsum("lk,kmcj->lmcj", own_rows, amplitude, precision=high)
    combined = jnp.concatenate([plain[:1], solved[None], plain[1:]], axis=0)
    scaled_growth = growth / (waves * (waves - 1))
    damping = 1.0 + diffusion[:, None, None] * (scaled_growth * scaled_growth)[None]
    return combined / damping[:, None, :, None, :]


chunks = 3
vmem_limit = 60 * 1024 * 1024


def split_table(table):
    high_part = np.asarray(table, jnp.bfloat16)
    low_part = np.asarray(table - high_part.astype(np.float64), jnp.bfloat16)
    return np.stack([high_part, low_part])


def fourier_tables(waves, longitudes, wave_count, scale):
    half = longitudes // 2
    per_wave = waves // wave_count
    synthesis, analysis = [], []
    for parity in range(2):
        order = np.arange(waves).reshape(wave_count * 2, per_wave // 4, 2)[:, :, parity]
        turns = order[:, :, None] * np.arange(half)[None, None, :] % longitudes
        angles = 2.0 * np.pi / longitudes * turns
        pair = np.stack([np.cos(angles), -np.sin(angles)], axis=1)
        factor = np.where(order == 0, 1.0, 2.0)[:, None, :, None]
        synthesis.append(split_table((pair * factor / scale).reshape(-1, half).T))
        analysis.append(split_table((pair / longitudes).reshape(-1, half)))
    return np.stack(synthesis), np.stack(analysis)


def halves(x):
    top = x.astype(jnp.bfloat16)
    return top, (x - top.astype(jnp.float32)).astype(jnp.bfloat16)


def dot3(left, right, dims):
    dot = lambda a, b: lax.dot_general(a, b, (dims, ((), ())), preferred_element_type=jnp.float32)
    return dot(left[0], right[0]) + (dot(left[0], right[1]) + dot(left[1], right[0]))


def kept(block, wave_index):
    degree = lax.broadcasted_iota(jnp.int32, block.shape, 1)
    return jnp.where(degree + wave_index < block.shape[1], block, 0.0)


def row_of(m, part, m_dev):
    half, quarter = m_dev // 2, m_dev // 4
    return m // half * m_dev + m % 2 * half + part * quarter + m % half // 2


send_octaves, send_top = 32, 5
back_octaves, back_top = 56, 24


def encode(x, octaves, top):
    floor_power = float(top - octaves)
    magnitude = jnp.abs(x)
    power = jnp.floor(jnp.log2(jnp.maximum(magnitude, 2.0**floor_power)))
    ratio = 250.0 / (octaves + 1)
    place = (magnitude * jnp.exp2(-power) + (power - floor_power)) * ratio
    step = jnp.floor(place)
    code = jnp.exp2(step - 125.0) * (place - step + 1.0)
    return jnp.where(x < 0.0, -code, code).astype(jnp.bfloat16)


def decode(code, octaves, top):
    floor_power = float(top - octaves)
    code = code.astype(jnp.float32)
    magnitude = jnp.abs(code)
    step = jnp.floor(jnp.log2(magnitude))
    place = (magnitude * jnp.exp2(-step) + (step + 124.0)) * ((octaves + 1) / 250.0)
    power = jnp.floor(place)
    lead = jnp.minimum(power, 1.0)
    value = (place - power + lead) * jnp.exp2(power - lead + floor_power)
    return jnp.where(code < 0.0, -value, value)


lanes = 128


def by_lanes(x):
    fields, lev, waves, parts, degrees = x.shape
    x = x.reshape(fields, lev, waves, parts, degrees // lanes, lanes).transpose(0, 1, 2, 4, 3, 5)
    return x.reshape(fields * lev, waves * (degrees // lanes) * parts, lanes)


def from_lanes(x, dims):
    fields, lev, waves, parts, degrees = dims
    x = x.reshape(fields, lev, waves, degrees // lanes, parts, lanes).transpose(0, 1, 2, 4, 3, 5)
    return x.reshape(dims)


def own_place():
    slabs = lax.axis_size("level")
    count = lax.axis_size("wave") * slabs
    return lax.axis_index("wave") * slabs + lax.axis_index("level"), count, slabs


def start_wave(src, dst, sems, at, sem):
    me, count, slabs = own_place()
    half = count // 2
    side = me // half

    def to(base, first):
        peer = base * half + lax.rem(me + first, half)
        pltpu.make_async_remote_copy(
            src_ref=src.at[at(peer)],
            dst_ref=dst.at[at(me)],
            send_sem=sems.at[0, sem],
            recv_sem=sems.at[1, sem],
            device_id=(peer // slabs, lax.rem(peer, slabs)),
            device_id_type=pl.DeviceIdType.MESH,
        ).start()
        return 0

    lax.fori_loop(0, half, lambda k, _: to(1 - side, k), 0)
    lax.fori_loop(1, half, lambda k, _: to(side, k), 0)


def wait_most(src, dst, sem, at, count):
    most = at(pl.ds(0, count - 1))
    pltpu.make_async_copy(src.at[most], dst.at[most], sem).wait()


def whole_block(x):
    return pl.BlockSpec(x.shape, lambda *_: (0,) * x.ndim)


def remote_params():
    return pltpu.CompilerParams(vmem_limit_bytes=vmem_limit, has_side_effects=True)


def twice_gelu(x):
    inner = x * (0.7978845608028654 + 0.7978845608028654 * 0.044715 * (x * x))
    return (x + x * jnp.tanh(inner)).astype(jnp.bfloat16)


def step_kernel(
    lat_ref, diff_ref, state_ref, leg_ref, modes_ref, rates_ref, gain_ref, b1_ref, b2_ref, b3_ref, perm_ref, syn_hbm, ana_hbm, w1_hbm, w2_hbm, w3_hbm,
    out_ref, swap_ref,
    band_ref, there_ref, here_ref, back_ref, home_ref, total_ref, hold_ref, modal_ref, gain_own, b3_own, syn_ref, ana_ref, w1_ref, w2_ref, w3_ref,
    there_sems, back_sems, swap_sems, load_sems,
):
    m_block, _, _, degrees = leg_ref.shape
    tiles = degrees // lanes
    fields, lev_dev = diff_ref.shape[0], hold_ref.shape[2]
    per_m = state_ref.shape[1] // m_block
    parts = per_m // tiles
    rows = back_ref.shape[0]
    step = pl.program_id(0)
    state_rows = state_ref.reshape(state_ref.shape[0] * state_ref.shape[1], lanes)
    out_rows = out_ref.reshape(out_ref.shape[0] * out_ref.shape[1], lanes)

    def place_of(f, i, c, t):
        return pl.ds(f * lev_dev * m_block * per_m + i * per_m + t * parts + c, lev_dev, stride=m_block * per_m)

    def put(f, i, c, value):
        for t in range(tiles):
            out_rows[place_of(f, i, c, t), :] = value[:, t * lanes : (t + 1) * lanes]

    first_steps = (pl.num_programs(0) - rows) // 2
    blocks = first_steps // chunks
    grid_steps = first_steps + rows
    m_dev = blocks * m_block
    feats = fields * lev_dev
    mc = m_dev * parts
    half = mc // 2
    me, count, slabs = own_place()
    waves = count // slabs
    width = slabs * feats
    per_chunk = rows // chunks
    level = lax.axis_index("level")
    loads = [
        pltpu.make_async_copy(src, dst, load_sems.at[i])
        for i, (src, dst) in enumerate(((syn_hbm, syn_ref), (ana_hbm, ana_ref), (w1_hbm, w1_ref), (w2_hbm, w2_ref), (w3_hbm, w3_ref)))
    ]

    @pl.when(step == blocks)
    def _():
        for load in loads:
            load.start()

    per_half = blocks // 2
    part_of = lambda h: pl.ds(pl.multiple_of(h * half, half), half)

    def there_at(sem):
        return lambda peer: (sem // 2, peer, slice(None), part_of(lax.rem(sem, 2)))

    def row_at(row):
        return lambda peer: (row, peer)

    def tail_at(sem):
        place = sem - (rows - per_chunk)
        return lambda peer: (rows - per_chunk + lax.rem(place, per_chunk), peer, part_of(place // per_chunk))

    @pl.when((step > 0) & (step <= first_steps) & (lax.rem(step, per_half) == 0))
    def _():
        sem = step // per_half - 1
        start_wave(there_ref, here_ref, there_sems, there_at(sem), sem)

    @pl.when(step == first_steps - 1)
    def _():
        for load in loads:
            load.wait()
        order = [slice((f * slabs + v) * lev_dev, (f * slabs + v + 1) * lev_dev) for v in range(slabs) for f in range(fields)]
        gain_own[...] = jnp.concatenate([gain_ref[:, at] for at in order], axis=1)
        b3_own[...] = jnp.concatenate([b3_ref[:, at] for at in order], axis=1)
        w3_ref[...] = jnp.concatenate([w3_ref[at, :] for at in order], axis=0) * 0.5
        w1_ref[...] = jnp.dot(w1_ref[...], perm_ref[...], preferred_element_type=jnp.float32).astype(jnp.bfloat16)
        w2_ref[...] = w2_ref[...] * 0.5
        same = lax.broadcasted_iota(jnp.int32, (width, width), 0) == lax.broadcasted_iota(jnp.int32, (width, width), 1)
        modal_ref[...] = same.astype(jnp.float32)
        total_ref[...] = jnp.zeros_like(total_ref)
        for v in range(slabs):
            for k in range(slabs):
                at = lambda i: slice(i * feats + lev_dev, i * feats + 2 * lev_dev)
                modal_ref[at(v), at(k)] = modes_ref[v * lev_dev : (v + 1) * lev_dev, k * lev_dev : (k + 1) * lev_dev]

    @pl.when(step < first_steps)
    def _():
        group, block = step // blocks, lax.rem(step, blocks)
        for i in range(m_block):
            m = block * m_block + i
            basis = leg_ref[i].reshape(-1, degrees)
            basis = halves(kept(basis, lax.axis_index("wave") * m_dev + m))
            coeffs = []
            for c in range(parts):
                pieces = [state_rows[pl.ds(i * per_m + t * parts + c, feats, stride=m_block * per_m), :] for t in range(tiles)]
                coeffs.append(jnp.concatenate(pieces, axis=1))
            coeffs = halves(jnp.concatenate(coeffs, axis=0))
            band = dot3(basis, coeffs, ((1,), (1,)))
            for c in range(parts):
                at = pl.ds(row_of(m, c, m_dev), band.shape[0], stride=mc)
                band_ref[at, :] = band[:, c * feats : (c + 1) * feats]

        @pl.when(lax.rem(block, per_half) == per_half - 1)
        def _():
            many = 4
            part = part_of(block // per_half)
            rows_of = band_ref.reshape(count, per_chunk, mc, feats)

            def one(k, _):
                at = pl.ds(k * many, many)
                there_ref[group, at, :, part] = encode(rows_of[at, :, part, :], send_octaves, send_top)
                return 0

            lax.fori_loop(0, count // many, one, 0)
            here_ref[group, me, :, part] = there_ref[group, me, :, part]

    @pl.when((step > first_steps) & (step <= grid_steps - per_chunk))
    def _():
        row = step - first_steps - 1
        start_wave(back_ref, home_ref, back_sems, row_at(row), row)

    @pl.when(step == grid_steps)
    def _():
        def tail(sem, _):
            start_wave(back_ref, home_ref, back_sems, tail_at(sem), sem)
            return 0

        lax.fori_loop(rows - per_chunk, rows + per_chunk, tail, 0)

    @pl.when((step >= first_steps) & (step < grid_steps))
    def _():
        row = step - first_steps
        group, place = row // per_chunk, lax.rem(row, per_chunk)

        @pl.when(place == 0)
        def _():
            for h in range(2):
                sem = 2 * group + h
                wait_most(there_ref, here_ref, there_sems.at[1, sem], there_at(sem), count)

        signs = []
        decoded = decode(here_ref[group, :, place], send_octaves, send_top).reshape(waves, slabs, 2, 2, half // 2, feats)
        for parity in range(2):
            band = [decoded[:, v, :, parity].reshape(waves * half, feats) for v in range(slabs)]
            band = halves(jnp.concatenate(band, axis=1))
            signs.append(dot3((syn_ref[parity, 0], syn_ref[parity, 1]), band, ((1,), (0,))))
        weight = lat_ref[group * (slabs * per_chunk) + level * per_chunk + place]
        updated = []
        for grid in (signs[0] + signs[1], signs[0] - signs[1]):
            values = grid.astype(jnp.bfloat16).astype(jnp.float32)
            inverse_rms = lax.rsqrt(jnp.mean(values * values, axis=1, keepdims=True) + norm_eps)
            normed = (values * inverse_rms * gain_own[...]).astype(jnp.bfloat16)
            hidden = twice_gelu(contract_last(normed, w1_ref[...]) + b1_ref[...])
            hidden = twice_gelu(contract_last(hidden, w2_ref[...]) + b2_ref[...])
            tendency = (contract_last(hidden, w3_ref[...]) + b3_own[...]).astype(jnp.bfloat16)
            updated.append((grid + tendency.astype(jnp.float32)) * weight)
        folded = (updated[0] + updated[1], updated[0] - updated[1])
        modal = halves(modal_ref[...])
        lane = lax.broadcasted_iota(jnp.int32, (waves * half, feats), 1)
        line = lax.rem(lax.broadcasted_iota(jnp.int32, (waves * half, feats), 0), half // 2) // (half // 4)
        swapped = (lane >= lev_dev) & (lane < 2 * lev_dev)
        sent = []
        for parity in range(2):
            wave = dot3((ana_ref[parity, 0], ana_ref[parity, 1]), halves(folded[parity]), ((1,), (0,)))
            wave = dot3(halves(wave), modal, ((1,), (0,)))
            slab = [wave[:, v * feats : (v + 1) * feats] for v in range(slabs)]
            turned = []
            for v in range(slabs):
                other = slab[1 - v].reshape(waves * 2, half // 2, feats)
                other = pltpu.roll(other, half // 4, 1).reshape(waves * half, feats)
                turned.append(jnp.where(swapped & (line == 1 - v), other, slab[v]).reshape(waves, 2, half // 2, feats))
            sent.append(turned)
        for v in range(slabs):
            both = jnp.concatenate([sent[0][v], sent[1][v]], axis=2).reshape(waves, mc, feats)
            both = encode(both, back_octaves, back_top)
            for w in range(waves):
                back_ref[row, w * slabs + v] = both[w]
        home_ref[row, me] = back_ref[row, me]

    late = step - grid_steps
    late_group, late_block = late // blocks, lax.rem(late, blocks)

    wave_ref = band_ref.reshape(count, per_chunk, mc, feats)

    @pl.when((step >= grid_steps) & (late_group < chunks - 1) & (late_block == 0))
    def _():
        def one(r, _):
            row = late_group * per_chunk + r
            wait_most(back_ref, home_ref, back_sems.at[1, row], row_at(row), count)
            wave_ref[:, r] = decode(home_ref[row], back_octaves, back_top)
            return 0

        lax.fori_loop(0, per_chunk, one, 0)

    @pl.when((step >= grid_steps) & (late_group == chunks - 1) & (lax.rem(late_block, per_half) == 0))
    def _():
        h = late_block // per_half

        def one(r, _):
            row = rows - per_chunk + r
            sem = row + h * per_chunk
            wait_most(back_ref, home_ref, back_sems.at[1, sem], tail_at(sem), count)
            wave_ref[:, r, part_of(h)] = decode(home_ref[row, :, part_of(h)], back_octaves, back_top)
            return 0

        lax.fori_loop(0, per_chunk, one, 0)

    def analysed(i):
        m = late_block * m_block + i
        basis = leg_ref[i].reshape(-1, degrees)
        basis = halves(kept(basis, lax.axis_index("wave") * m_dev + m))
        wave = [band_ref[pl.ds(row_of(m, c, m_dev), basis[0].shape[0], stride=mc), :] for c in range(parts)]
        return m, dot3(halves(jnp.concatenate(wave, axis=1)), basis, ((0,), (0,)))

    @pl.when((step >= grid_steps) & (late_group < chunks - 1))
    def _():
        for i in range(m_block):
            m, part = analysed(i)
            total_ref[m] = total_ref[m] + part

    def swap(at):
        return pltpu.make_async_remote_copy(
            src_ref=hold_ref.at[at],
            dst_ref=swap_ref.at[at],
            send_sem=swap_sems.at[0, at],
            recv_sem=swap_sems.at[1, at],
            device_id=(lax.axis_index("wave"), 1 - level),
            device_id_type=pl.DeviceIdType.MESH,
        )

    @pl.when((step >= grid_steps) & (late_group == chunks - 1))
    def _():
        own = halves(modes_ref[pl.ds(pl.multiple_of(level * lev_dev, 8), lev_dev), :])
        other = halves(modes_ref[pl.ds(pl.multiple_of((1 - level) * lev_dev, 8), lev_dev), :])
        for i in range(m_block):
            m, part = analysed(i)
            spectral = total_ref[m] + part
            degree = lax.axis_index("wave") * m_dev + m + lax.broadcasted_iota(jnp.int32, (1, degrees), 1)
            growth = (degree * (degree + 1)).astype(jnp.float32)
            scaled_growth = growth / (degrees * (degrees - 1))
            square = scaled_growth * scaled_growth
            for f in range(fields):
                if f != 1:
                    inverse = 1.0 / (1.0 + diff_ref[f] * square)
                    for c in range(parts):
                        first = c * feats + f * lev_dev
                        put(f, i, c, spectral[first : first + lev_dev] * inverse)
            modal = [spectral[c * feats + lev_dev : c * feats + 2 * lev_dev] for c in range(parts)]
            rates = lax.dot_general(
                rates_ref[...], growth, (((0,), (0,)), ((), ())), precision=lax.Precision.HIGHEST, preferred_element_type=jnp.float32
            )
            amplitude = halves(jnp.concatenate(modal, axis=0) / (1.0 + rates))
            inverse = 1.0 / (1.0 + diff_ref[1] * square)
            mine = dot3(own, amplitude, ((1,), (0,))) * inverse
            for c in range(parts):
                put(1, i, c, mine)
            hold_ref[late_block, i] = encode(dot3(other, amplitude, ((1,), (0,))) * inverse, back_octaves, back_top)
        swap(late_block).start()

    @pl.when(step == pl.num_programs(0) - 1)
    def _():
        lax.fori_loop(0, 2 * chunks, lambda at, _: (wait_most(there_ref, here_ref, there_sems.at[0, at], there_at(at), count), 0)[1], 0)
        lax.fori_loop(0, rows - per_chunk, lambda at, _: (wait_most(back_ref, home_ref, back_sems.at[0, at], row_at(at), count), 0)[1], 0)
        lax.fori_loop(rows - per_chunk, rows + per_chunk, lambda at, _: (wait_most(back_ref, home_ref, back_sems.at[0, at], tail_at(at), count), 0)[1], 0)
        lax.fori_loop(0, blocks, lambda at, _: (swap(at).wait(), 0)[1], 0)


def whole_step(state, legendre, lat, diffusion, modes, rates, gain, b1, b2, b3, perm, synthesis, analysis, w1, w2, w3):
    fields, lev_dev, m_dev, parts, degrees = state.shape
    waves, slabs = lax.axis_size("wave"), lax.axis_size("level")
    count, feats, mc = waves * slabs, fields * lev_dev, m_dev * parts
    tile = legendre.shape[1] // (waves * chunks)
    legendre = legendre.reshape(m_dev, waves, chunks, tile, degrees)
    per_chunk = tile // slabs
    rows = chunks * per_chunk
    m_block = 4
    blocks = m_dev // m_block
    first_steps = chunks * blocks
    last = first_steps - 1
    grid_steps = first_steps + rows
    there = (chunks, count, per_chunk, mc, feats)
    back = (rows, count, mc, feats)
    small = (modes, rates, gain, b1, b2, b3, perm)
    large = (synthesis, analysis, w1, w2, w3)
    swap = (blocks, m_block, lev_dev, degrees)
    lined = by_lanes(state)
    line_block = (lined.shape[0], lined.shape[1] // blocks, lanes)
    any_spec = pl.BlockSpec(memory_space=pl.ANY)
    smem = pl.BlockSpec(memory_space=pltpu.SMEM)
    bf16, f32 = jnp.bfloat16, jnp.float32
    pair = lambda i: jnp.where(i < first_steps, i, jnp.maximum(i - grid_steps, 0))
    return pl.pallas_call(
        step_kernel,
        grid=(grid_steps + first_steps,),
        out_shape=(jax.ShapeDtypeStruct(lined.shape, f32), jax.ShapeDtypeStruct(swap, bf16)),
        in_specs=[
            smem,
            smem,
            pl.BlockSpec(line_block, lambda i: (0, jnp.minimum(i, last) % blocks, 0)),
            pl.BlockSpec((m_block, waves, None, tile, degrees), lambda i: (pair(i) % blocks, 0, pair(i) // blocks, 0, 0)),
            *[whole_block(x) for x in small],
            *[any_spec for _ in large],
        ],
        out_specs=(
            pl.BlockSpec(line_block, lambda i: (0, jnp.maximum(i - (grid_steps + first_steps - blocks), 0), 0)),
            any_spec,
        ),
        scratch_shapes=[
            pltpu.VMEM((count * per_chunk * mc, feats), f32),
            pltpu.VMEM(there, bf16),
            pltpu.VMEM(there, bf16),
            pltpu.VMEM(back, bf16),
            pltpu.VMEM(back, bf16),
            pltpu.VMEM((m_dev, parts * feats, degrees), f32),
            pltpu.VMEM(swap, bf16),
            pltpu.VMEM((slabs * feats, slabs * feats), f32),
            pltpu.VMEM(gain.shape, f32),
            pltpu.VMEM(b3.shape, f32),
            *[pltpu.VMEM(x.shape, bf16) for x in large],
            pltpu.SemaphoreType.DMA((2, 2 * chunks)),
            pltpu.SemaphoreType.DMA((2, rows + per_chunk)),
            pltpu.SemaphoreType.DMA((2, blocks)),
            pltpu.SemaphoreType.DMA((len(large),)),
        ],
        compiler_params=remote_params(),
    )(lat, diffusion, lined, legendre, *small, *large)


def merge_kernel(parts, old_ref, got_ref, out_ref):
    lev_dev, per_lev, _ = out_ref.shape
    blocks, m_block, _, degrees = got_ref.shape
    tiles = degrees // lanes
    other = 1 - lax.axis_index("level")
    out_ref[...] = old_ref[...]

    @pl.when(pl.program_id(0) == 1)
    def _():
        out_rows = out_ref.reshape(lev_dev * per_lev, lanes)
        for b in range(blocks):
            for i in range(m_block):
                value = decode(got_ref[b, i], back_octaves, back_top)
                for t in range(tiles):
                    at = ((b * m_block + i) * tiles + t) * parts + other
                    out_rows[pl.ds(at, lev_dev, stride=per_lev), :] = value[:, t * lanes : (t + 1) * lanes]


def merge_step(fields, parts, lined, got):
    block = pl.BlockSpec((lined.shape[0] // fields, *lined.shape[1:]), lambda i: (i, 0, 0))
    return pl.pallas_call(
        functools.partial(merge_kernel, parts),
        grid=(fields,),
        out_shape=jax.ShapeDtypeStruct(lined.shape, jnp.float32),
        in_specs=[block, whole_block(got)],
        out_specs=block,
    )(lined, got)


def fast_body(longitudes, state, legendre, lat_weight, modes, mode_rates, diffusion, norm_gain, w_first, b_first, w_second, b_second, w_third, b_third):
    fields, lev_dev, m_dev, parts, degrees = state.shape
    levels = modes.shape[0]
    wave_count, level_count = lax.axis_size("wave"), lax.axis_size("level")
    synthesis, analysis = fourier_tables(degrees, longitudes, wave_count, 1.0)
    place = np.arange(fields * levels).reshape(fields, level_count, lev_dev).swapaxes(0, 1).reshape(-1)
    perm = np.zeros((fields * levels, fields * levels), jnp.bfloat16)
    perm[place, np.arange(fields * levels)] = 1.0
    out, got = whole_step(
        state,
        legendre,
        lat_weight,
        diffusion,
        modes,
        mode_rates[None],
        norm_gain[None],
        b_first[None],
        b_second[None],
        b_third[None],
        perm,
        synthesis,
        analysis,
        w_first,
        w_second,
        w_third,
    )
    return from_lanes(merge_step(fields, parts, out, got), state.shape)


def solution(mesh):
    wave_count, level_count = mesh.shape["wave"], mesh.shape["level"]

    def step(state, legendre, *rest):
        longitudes = 2 * legendre.shape[1]
        fields, levels, waves, _, degrees = state.shape
        fits = (
            level_count == 2
            and waves % (16 * wave_count) == 0
            and fields * levels % (128 * level_count) == 0
            and levels % (8 * level_count) == 0
            and legendre.shape[1] % (8 * chunks * wave_count) == 0
            and degrees % 128 == 0
        )
        mapped = jax.shard_map(
            functools.partial(fast_body if fits else general_body, longitudes),
            mesh=mesh,
            in_specs=(P(None, "level", "wave", None, None), P("wave", None, None), P("wave")) + (P(),) * 10,
            out_specs=P(None, "level", "wave", None, None),
            check_vma=False,
        )
        return mapped(state, legendre, *rest)

    return step
```

```python
import functools
import math

import jax
import jax.numpy as jnp
import numpy as np
from jax import lax
from jax.experimental import pallas as pl
from jax.experimental.pallas import tpu as pltpu
from jax.sharding import PartitionSpec as P

high = lax.Precision.HIGH
norm_eps = 1e-06
axes = ("wave", "level")
send_scale = 1024.0


def phase_angles(waves, longitudes):
    wave_idx = jnp.arange(waves, dtype=jnp.int32)
    lon_idx = jnp.arange(longitudes, dtype=jnp.int32)
    phase_turns = wave_idx[:, None] * lon_idx[None, :] % longitudes
    return (2.0 * jnp.pi / longitudes * phase_turns.astype(jnp.float32), wave_idx)


def synthesis_table(waves, longitudes):
    angle_table, wave_idx = phase_angles(waves, longitudes)
    factor = jnp.where(wave_idx == 0, 1.0, 2.0).astype(jnp.float32)[:, None]
    return jnp.stack([factor * jnp.cos(angle_table), -factor * jnp.sin(angle_table)], axis=1)


def analysis_table(waves, longitudes):
    angle_table, _ = phase_angles(waves, longitudes)
    return jnp.stack([jnp.cos(angle_table), -jnp.sin(angle_table)], axis=1) / longitudes


def contract_last(left, right):
    return lax.dot_general(
        left, right, (((1,), (1,)), ((), ())), preferred_element_type=jnp.float32
    )


def physics_kernel(grid_ref, lat_ref, gain_ref, w1_ref, b1_ref, w2_ref, b2_ref, w3_ref, b3_ref, out_ref, top_ref):
    grid_rows = grid_ref[0]
    values = grid_rows.astype(jnp.bfloat16).astype(jnp.float32)
    inverse_rms = lax.rsqrt(jnp.mean(values * values, axis=1, keepdims=True) + norm_eps)
    normed = (values * inverse_rms * gain_ref[...]).astype(jnp.bfloat16)
    hidden = jax.nn.gelu(contract_last(normed, w1_ref[...]) + b1_ref[...]).astype(jnp.bfloat16)
    hidden = jax.nn.gelu(contract_last(hidden, w2_ref[...]) + b2_ref[...]).astype(jnp.bfloat16)
    tendency = (contract_last(hidden, w3_ref[...]) + b3_ref[...]).astype(jnp.bfloat16)
    updated = (grid_rows + tendency.astype(jnp.float32)) * lat_ref[pl.program_id(0)]
    out_ref[0] = updated
    top_ref[0] = jnp.max(jnp.abs(updated), axis=0, keepdims=True)


def column_step(grid, lat, gain, w1, b1, w2, b2, w3, b3):
    rows, lon, feats = grid.shape
    hid = w1.shape[0]
    whole = lambda *shape: pl.BlockSpec(shape, lambda i: (0,) * len(shape))
    block = pl.BlockSpec((1, lon, feats), lambda i: (i, 0, 0))
    return pl.pallas_call(
        physics_kernel,
        grid=(rows,),
        out_shape=(
            jax.ShapeDtypeStruct((rows, lon, feats), jnp.float32),
            jax.ShapeDtypeStruct((rows, 1, feats), jnp.float32),
        ),
        in_specs=[
            block,
            pl.BlockSpec(memory_space=pltpu.SMEM),
            whole(1, feats),
            whole(hid, feats),
            whole(1, hid),
            whole(hid, hid),
            whole(1, hid),
            whole(feats, hid),
            whole(1, feats),
        ],
        out_specs=(block, pl.BlockSpec((1, 1, feats), lambda i: (i, 0, 0))),
        compiler_params=pltpu.CompilerParams(vmem_limit_bytes=56 * 1024 * 1024),
    )(grid, lat, gain[None], w1, b1[None], w2, b2[None], w3, b3[None])


def general_body(
    longitudes,
    state,
    legendre,
    lat_weight,
    modes,
    mode_rates,
    diffusion,
    norm_gain,
    w_first,
    b_first,
    w_second,
    b_second,
    w_third,
    b_third,
):
    fields, lev_dev, m_dev, parts, degrees = state.shape
    levels = modes.shape[0]
    waves = degrees
    wave_count = lax.axis_size("wave")
    level_count = lax.axis_size("level")
    lat_band = lat_weight.shape[0]
    lat_own = -(-lat_band // level_count)
    lat_extra = lat_own * level_count - lat_band
    wave_global = lax.axis_index("wave") * m_dev + jnp.arange(m_dev, dtype=jnp.int32)
    degree_index = wave_global[:, None] + jnp.arange(degrees, dtype=jnp.int32)[None, :]
    kept_mask = (degree_index < waves).astype(jnp.float32)
    basis = legendre * kept_mask[:, None, :]
    if lat_extra:
        basis = basis.reshape(m_dev, wave_count, lat_band, degrees)
        basis = jnp.pad(basis, ((0, 0), (0, 0), (0, lat_extra), (0, 0)))
        basis = basis.reshape(m_dev, -1, degrees)
        lat_weight = jnp.pad(lat_weight, (0, lat_extra))
    inverse_tab = synthesis_table(waves, longitudes).reshape(wave_count, m_dev, parts, longitudes)
    forward_tab = analysis_table(waves, longitudes).reshape(wave_count, m_dev, parts, longitudes)

    band = jnp.einsum("flmcj,maj->amcfl", state, basis, precision=high)
    band = (band * send_scale).astype(jnp.float16)
    band = band.reshape(wave_count * level_count, lat_own, m_dev, parts, fields, lev_dev)
    band = lax.all_to_all(band, axes, split_axis=0, concat_axis=0, tiled=True)
    band = band.reshape(wave_count, level_count, lat_own, m_dev, parts, fields, lev_dev)
    band = band.astype(jnp.float32) * (1.0 / send_scale)
    grid = jnp.einsum("wvamcfl,wmco->aovfl", band, inverse_tab, precision=high)
    feats = fields * levels
    grid = grid.reshape(lat_own, longitudes, feats)

    def slabs_first(x):
        split = x.reshape((fields, level_count, lev_dev) + x.shape[1:])
        return jnp.swapaxes(split, 0, 1).reshape(x.shape)

    lat = lax.dynamic_slice_in_dim(lat_weight, lax.axis_index("level") * lat_own, lat_own, 0)
    updated, tops = column_step(
        grid,
        lat,
        slabs_first(norm_gain),
        slabs_first(w_first.T).T,
        b_first,
        w_second,
        b_second,
        slabs_first(w_third),
        slabs_first(b_third),
    )
    top = jnp.maximum(jnp.max(tops), 1e-25)
    reach = 32768.0 / levels**0.5
    tops_all = lax.all_gather(top / reach, axes).reshape(wave_count, level_count)

    wave = jnp.einsum("aok,wmco->wmcak", updated, forward_tab, precision=high)
    wave = wave * (reach / top)
    wave = wave.reshape(wave_count, m_dev, parts, lat_own, level_count, fields, lev_dev)
    modal = jnp.einsum(
        "wmcavl,vlk->wmcak",
        wave[..., 1, :],
        modes.reshape(level_count, lev_dev, levels),
        precision=high,
    )
    others = jnp.concatenate([wave[..., :1, :], wave[..., 2:, :]], axis=-2)
    others = others.reshape(wave_count, m_dev, parts, lat_own, level_count, (fields - 1) * lev_dev)
    others = jnp.moveaxis(others, 4, 1)
    modal = jnp.broadcast_to(modal[:, None], others.shape[:-1] + (levels,))
    sent = jnp.concatenate([others, modal], axis=-1).astype(jnp.float16)
    sent = sent.reshape((wave_count * level_count,) + sent.shape[2:])
    got = lax.all_to_all(sent, axes, split_axis=0, concat_axis=0, tiled=True)
    got = got.reshape((wave_count, level_count) + got.shape[1:]).astype(jnp.float32)
    got = got * tops_all[:, :, None, None, None, None]
    basis_split = basis.reshape(m_dev, wave_count, level_count, lat_own, degrees)
    spectral = jnp.einsum("wvmcaq,mwvaj->qmcj", got, basis_split, precision=high)

    growth = (degree_index * (degree_index + 1)).astype(jnp.float32)
    plain = spectral[: (fields - 1) * lev_dev].reshape(fields - 1, lev_dev, m_dev, parts, degrees)
    divisor = 1.0 + mode_rates[:, None, None, None] * growth[None, :, None, :]
    amplitude = spectral[(fields - 1) * lev_dev :] / divisor
    own_rows = lax.dynamic_slice_in_dim(modes, lax.axis_index("level") * lev_dev, lev_dev, 0)
    solved = jnp.einsum("lk,kmcj->lmcj", own_rows, amplitude, precision=high)
    combined = jnp.concatenate([plain[:1], solved[None], plain[1:]], axis=0)
    scaled_growth = growth / (waves * (waves - 1))
    damping = 1.0 + diffusion[:, None, None] * (scaled_growth * scaled_growth)[None]
    return combined / damping[:, None, :, None, :]


chunks = 3
vmem_limit = 60 * 1024 * 1024


def split_table(table):
    high_part = np.asarray(table, jnp.bfloat16)
    low_part = np.asarray(table - high_part.astype(np.float64), jnp.bfloat16)
    return np.stack([high_part, low_part])


def fourier_tables(waves, longitudes, wave_count, scale):
    half = longitudes // 2
    per_wave = waves // wave_count
    synthesis, analysis = [], []
    for parity in range(2):
        order = np.arange(waves).reshape(wave_count * 2, per_wave // 4, 2)[:, :, parity]
        turns = order[:, :, None] * np.arange(half)[None, None, :] % longitudes
        angles = 2.0 * np.pi / longitudes * turns
        pair = np.stack([np.cos(angles), -np.sin(angles)], axis=1)
        factor = np.where(order == 0, 1.0, 2.0)[:, None, :, None]
        synthesis.append(split_table((pair * factor / scale).reshape(-1, half).T))
        analysis.append(split_table((pair / longitudes).reshape(-1, half)))
    return np.stack(synthesis), np.stack(analysis)


def halves(x):
    top = x.astype(jnp.bfloat16)
    return top, (x - top.astype(jnp.float32)).astype(jnp.bfloat16)


def dot3(left, right, dims):
    dot = lambda a, b: lax.dot_general(a, b, (dims, ((), ())), preferred_element_type=jnp.float32)
    return dot(left[0], right[0]) + (dot(left[0], right[1]) + dot(left[1], right[0]))


def kept(block, wave_index):
    degree = lax.broadcasted_iota(jnp.int32, block.shape, 1)
    return jnp.where(degree + wave_index < block.shape[1], block, 0.0)


def row_of(m, part, m_dev):
    half, quarter = m_dev // 2, m_dev // 4
    return m // half * m_dev + m % 2 * half + part * quarter + m % half // 2


send_octaves, send_top = 32, 5
back_octaves, back_top = 56, 24


def encode(x, octaves, top):
    floor_power = float(top - octaves)
    magnitude = jnp.abs(x)
    power = jnp.floor(jnp.log2(jnp.maximum(magnitude, 2.0**floor_power)))
    ratio = 250.0 / (octaves + 1)
    place = (magnitude * jnp.exp2(-power) + (power - floor_power)) * ratio
    step = jnp.floor(place)
    code = jnp.exp2(step - 125.0) * (place - step + 1.0)
    return jnp.where(x < 0.0, -code, code).astype(jnp.bfloat16)


def decode(code, octaves, top):
    floor_power = float(top - octaves)
    code = code.astype(jnp.float32)
    magnitude = jnp.abs(code)
    step = jnp.floor(jnp.log2(magnitude))
    place = (magnitude * jnp.exp2(-step) + (step + 124.0)) * ((octaves + 1) / 250.0)
    power = jnp.floor(place)
    lead = jnp.minimum(power, 1.0)
    value = (place - power + lead) * jnp.exp2(power - lead + floor_power)
    return jnp.where(code < 0.0, -value, value)


lanes = 128


def by_lanes(x):
    fields, lev, waves, parts, degrees = x.shape
    x = x.reshape(fields, lev, waves, parts, degrees // lanes, lanes).transpose(0, 1, 2, 4, 3, 5)
    return x.reshape(fields * lev, waves * (degrees // lanes) * parts, lanes)


def from_lanes(x, dims):
    fields, lev, waves, parts, degrees = dims
    x = x.reshape(fields, lev, waves, degrees // lanes, parts, lanes).transpose(0, 1, 2, 4, 3, 5)
    return x.reshape(dims)


def own_place():
    slabs = lax.axis_size("level")
    count = lax.axis_size("wave") * slabs
    return lax.axis_index("wave") * slabs + lax.axis_index("level"), count, slabs


def start_wave(src, dst, sems, at, sem):
    me, count, slabs = own_place()
    half = count // 2
    side = me // half

    def to(base, first):
        peer = base * half + lax.rem(me + first, half)
        pltpu.make_async_remote_copy(
            src_ref=src.at[at(peer)],
            dst_ref=dst.at[at(me)],
            send_sem=sems.at[0, sem],
            recv_sem=sems.at[1, sem],
            device_id=(peer // slabs, lax.rem(peer, slabs)),
            device_id_type=pl.DeviceIdType.MESH,
        ).start()
        return 0

    lax.fori_loop(0, half, lambda k, _: to(1 - side, k), 0)
    lax.fori_loop(1, half, lambda k, _: to(side, k), 0)


def wait_most(src, dst, sem, at, count):
    most = at(pl.ds(0, count - 1))
    pltpu.make_async_copy(src.at[most], dst.at[most], sem).wait()


def whole_block(x):
    return pl.BlockSpec(x.shape, lambda *_: (0,) * x.ndim)


def remote_params():
    return pltpu.CompilerParams(vmem_limit_bytes=vmem_limit, has_side_effects=True)


def twice_gelu(x):
    inner = x * (0.7978845608028654 + 0.7978845608028654 * 0.044715 * (x * x))
    return (x + x * jnp.tanh(inner)).astype(jnp.bfloat16)


def step_kernel(
    lat_ref, diff_ref, state_ref, leg_ref, modes_ref, rates_ref, gain_ref, b1_ref, b2_ref, b3_ref, perm_ref, syn_hbm, ana_hbm, w1_hbm, w2_hbm, w3_hbm,
    out_ref, swap_ref,
    band_ref, there_ref, here_ref, back_ref, home_ref, total_ref, hold_ref, modal_ref, gain_own, b3_own, syn_ref, ana_ref, w1_ref, w2_ref, w3_ref,
    there_sems, back_sems, swap_sems, load_sems,
):
    m_block, _, _, degrees = leg_ref.shape
    tiles = degrees // lanes
    fields, lev_dev = diff_ref.shape[0], hold_ref.shape[2]
    per_m = state_ref.shape[1] // m_block
    parts = per_m // tiles
    rows = back_ref.shape[0]
    step = pl.program_id(0)
    state_rows = state_ref.reshape(state_ref.shape[0] * state_ref.shape[1], lanes)
    out_rows = out_ref.reshape(out_ref.shape[0] * out_ref.shape[1], lanes)

    def place_of(f, i, c, t):
        return pl.ds(f * lev_dev * m_block * per_m + i * per_m + t * parts + c, lev_dev, stride=m_block * per_m)

    def put(f, i, c, value):
        for t in range(tiles):
            out_rows[place_of(f, i, c, t), :] = value[:, t * lanes : (t + 1) * lanes]

    first_steps = (pl.num_programs(0) - rows) // 2
    blocks = first_steps // chunks
    grid_steps = first_steps + rows
    m_dev = blocks * m_block
    feats = fields * lev_dev
    mc = m_dev * parts
    half = mc // 2
    me, count, slabs = own_place()
    waves = count // slabs
    width = slabs * feats
    per_chunk = rows // chunks
    level = lax.axis_index("level")
    loads = [
        pltpu.make_async_copy(src, dst, load_sems.at[i])
        for i, (src, dst) in enumerate(((syn_hbm, syn_ref), (ana_hbm, ana_ref), (w1_hbm, w1_ref), (w2_hbm, w2_ref), (w3_hbm, w3_ref)))
    ]

    @pl.when(step == blocks)
    def _():
        for load in loads:
            load.start()

    per_half = blocks // 2
    part_of = lambda h: pl.ds(pl.multiple_of(h * half, half), half)

    def there_at(sem):
        return lambda peer: (sem // 2, lax.rem(sem, 2), peer)

    def row_at(row):
        return lambda peer: (row, peer)

    def tail_at(sem):
        place = sem - (rows - per_chunk)
        return lambda peer: (rows - per_chunk + lax.rem(place, per_chunk), peer, part_of(place // per_chunk))

    @pl.when((step > 0) & (step <= first_steps) & (lax.rem(step, per_half) == 0))
    def _():
        sem = step // per_half - 1
        start_wave(there_ref, here_ref, there_sems, there_at(sem), sem)

    @pl.when(step == first_steps - 1)
    def _():
        for load in loads:
            load.wait()
        order = [slice((f * slabs + v) * lev_dev, (f * slabs + v + 1) * lev_dev) for v in range(slabs) for f in range(fields)]
        gain_own[...] = jnp.concatenate([gain_ref[:, at] for at in order], axis=1)
        b3_own[...] = jnp.concatenate([b3_ref[:, at] for at in order], axis=1)
        w3_ref[...] = jnp.concatenate([w3_ref[at, :] for at in order], axis=0) * 0.5
        w1_ref[...] = jnp.dot(w1_ref[...], perm_ref[...], preferred_element_type=jnp.float32).astype(jnp.bfloat16)
        w2_ref[...] = w2_ref[...] * 0.5
        same = lax.broadcasted_iota(jnp.int32, (width, width), 0) == lax.broadcasted_iota(jnp.int32, (width, width), 1)
        modal_ref[...] = same.astype(jnp.float32)
        total_ref[...] = jnp.zeros_like(total_ref)
        for v in range(slabs):
            for k in range(slabs):
                at = lambda i: slice(i * feats + lev_dev, i * feats + 2 * lev_dev)
                modal_ref[at(v), at(k)] = modes_ref[v * lev_dev : (v + 1) * lev_dev, k * lev_dev : (k + 1) * lev_dev]

    @pl.when(step < first_steps)
    def _():
        group, block = step // blocks, lax.rem(step, blocks)
        for i in range(m_block):
            m = block * m_block + i
            basis = leg_ref[i].reshape(-1, degrees)
            basis = halves(kept(basis, lax.axis_index("wave") * m_dev + m))
            coeffs = []
            for c in range(parts):
                pieces = [state_rows[pl.ds(i * per_m + t * parts + c, feats, stride=m_block * per_m), :] for t in range(tiles)]
                coeffs.append(jnp.concatenate(pieces, axis=1))
            coeffs = halves(jnp.concatenate(coeffs, axis=0))
            band = dot3(basis, coeffs, ((1,), (1,)))
            for c in range(parts):
                at = pl.ds(row_of(m, c, m_dev), band.shape[0], stride=mc)
                band_ref[at, :] = band[:, c * feats : (c + 1) * feats]

        @pl.when(lax.rem(block, per_half) == per_half - 1)
        def _():
            many = 4
            h = block // per_half
            part = part_of(h)
            rows_of = band_ref.reshape(count, per_chunk, mc, feats)

            def one(k, _):
                at = pl.ds(k * many, many)
                there_ref[group, h, at] = encode(rows_of[at, :, part, :], send_octaves, send_top)
                return 0

            lax.fori_loop(0, count // many, one, 0)
            here_ref[group, h, me] = there_ref[group, h, me]

    @pl.when((step > first_steps) & (step <= grid_steps - per_chunk))
    def _():
        row = step - first_steps - 1
        start_wave(back_ref, home_ref, back_sems, row_at(row), row)

    @pl.when(step == grid_steps)
    def _():
        def tail(sem, _):
            start_wave(back_ref, home_ref, back_sems, tail_at(sem), sem)
            return 0

        lax.fori_loop(rows - per_chunk, rows + per_chunk, tail, 0)

    @pl.when((step >= first_steps) & (step < grid_steps))
    def _():
        row = step - first_steps
        group, place = row // per_chunk, lax.rem(row, per_chunk)

        @pl.when(place == 0)
        def _():
            for h in range(2):
                sem = 2 * group + h
                wait_most(there_ref, here_ref, there_sems.at[1, sem], there_at(sem), count)

        signs = []
        decoded = [decode(here_ref[group, h, :, place], send_octaves, send_top).reshape(waves, slabs, 2, half // 2, feats) for h in range(2)]
        for parity in range(2):
            band = [jnp.concatenate([d[:, v, parity] for d in decoded], axis=1).reshape(waves * half, feats) for v in range(slabs)]
            band = halves(jnp.concatenate(band, axis=1))
            signs.append(dot3((syn_ref[parity, 0], syn_ref[parity, 1]), band, ((1,), (0,))))
        weight = lat_ref[group * (slabs * per_chunk) + level * per_chunk + place]
        updated = []
        for grid in (signs[0] + signs[1], signs[0] - signs[1]):
            values = grid.astype(jnp.bfloat16).astype(jnp.float32)
            inverse_rms = lax.rsqrt(jnp.mean(values * values, axis=1, keepdims=True) + norm_eps)
            normed = (values * inverse_rms * gain_own[...]).astype(jnp.bfloat16)
            hidden = twice_gelu(contract_last(normed, w1_ref[...]) + b1_ref[...])
            hidden = twice_gelu(contract_last(hidden, w2_ref[...]) + b2_ref[...])
            tendency = (contract_last(hidden, w3_ref[...]) + b3_own[...]).astype(jnp.bfloat16)
            updated.append((grid + tendency.astype(jnp.float32)) * weight)
        folded = (updated[0] + updated[1], updated[0] - updated[1])
        modal = halves(modal_ref[...])
        lane = lax.broadcasted_iota(jnp.int32, (waves * half, feats), 1)
        line = lax.rem(lax.broadcasted_iota(jnp.int32, (waves * half, feats), 0), half // 2) // (half // 4)
        swapped = (lane >= lev_dev) & (lane < 2 * lev_dev)
        sent = []
        for parity in range(2):
            wave = dot3((ana_ref[parity, 0], ana_ref[parity, 1]), halves(folded[parity]), ((1,), (0,)))
            wave = dot3(halves(wave), modal, ((1,), (0,)))
            slab = [wave[:, v * feats : (v + 1) * feats] for v in range(slabs)]
            turned = []
            for v in range(slabs):
                other = slab[1 - v].reshape(waves * 2, half // 2, feats)
                other = pltpu.roll(other, half // 4, 1).reshape(waves * half, feats)
                turned.append(jnp.where(swapped & (line == 1 - v), other, slab[v]).reshape(waves, 2, half // 2, feats))
            sent.append(turned)
        for v in range(slabs):
            both = jnp.concatenate([sent[0][v], sent[1][v]], axis=2).reshape(waves, mc, feats)
            both = encode(both, back_octaves, back_top)
            for w in range(waves):
                back_ref[row, w * slabs + v] = both[w]
        home_ref[row, me] = back_ref[row, me]

    late = step - grid_steps
    late_group, late_block = late // blocks, lax.rem(late, blocks)

    wave_ref = band_ref.reshape(count, per_chunk, mc, feats)

    @pl.when((step >= grid_steps) & (late_group < chunks - 1) & (late_block == 0))
    def _():
        def one(r, _):
            row = late_group * per_chunk + r
            wait_most(back_ref, home_ref, back_sems.at[1, row], row_at(row), count)
            wave_ref[:, r] = decode(home_ref[row], back_octaves, back_top)
            return 0

        lax.fori_loop(0, per_chunk, one, 0)

    @pl.when((step >= grid_steps) & (late_group == chunks - 1) & (lax.rem(late_block, per_half) == 0))
    def _():
        h = late_block // per_half

        def one(r, _):
            row = rows - per_chunk + r
            sem = row + h * per_chunk
            wait_most(back_ref, home_ref, back_sems.at[1, sem], tail_at(sem), count)
            wave_ref[:, r, part_of(h)] = decode(home_ref[row, :, part_of(h)], back_octaves, back_top)
            return 0

        lax.fori_loop(0, per_chunk, one, 0)

    def analysed(i):
        m = late_block * m_block + i
        basis = leg_ref[i].reshape(-1, degrees)
        basis = halves(kept(basis, lax.axis_index("wave") * m_dev + m))
        wave = [band_ref[pl.ds(row_of(m, c, m_dev), basis[0].shape[0], stride=mc), :] for c in range(parts)]
        return m, dot3(halves(jnp.concatenate(wave, axis=1)), basis, ((0,), (0,)))

    @pl.when((step >= grid_steps) & (late_group < chunks - 1))
    def _():
        for i in range(m_block):
            m, part = analysed(i)
            total_ref[m] = total_ref[m] + part

    def swap(at):
        return pltpu.make_async_remote_copy(
            src_ref=hold_ref.at[at],
            dst_ref=swap_ref.at[at],
            send_sem=swap_sems.at[0, at],
            recv_sem=swap_sems.at[1, at],
            device_id=(lax.axis_index("wave"), 1 - level),
            device_id_type=pl.DeviceIdType.MESH,
        )

    @pl.when((step >= grid_steps) & (late_group == chunks - 1))
    def _():
        own = halves(modes_ref[pl.ds(pl.multiple_of(level * lev_dev, 8), lev_dev), :])
        other = halves(modes_ref[pl.ds(pl.multiple_of((1 - level) * lev_dev, 8), lev_dev), :])
        for i in range(m_block):
            m, part = analysed(i)
            spectral = total_ref[m] + part
            degree = lax.axis_index("wave") * m_dev + m + lax.broadcasted_iota(jnp.int32, (1, degrees), 1)
            growth = (degree * (degree + 1)).astype(jnp.float32)
            scaled_growth = growth / (degrees * (degrees - 1))
            square = scaled_growth * scaled_growth
            for f in range(fields):
                if f != 1:
                    inverse = 1.0 / (1.0 + diff_ref[f] * square)
                    for c in range(parts):
                        first = c * feats + f * lev_dev
                        put(f, i, c, spectral[first : first + lev_dev] * inverse)
            modal = [spectral[c * feats + lev_dev : c * feats + 2 * lev_dev] for c in range(parts)]
            rates = lax.dot_general(
                rates_ref[...], growth, (((0,), (0,)), ((), ())), precision=lax.Precision.HIGHEST, preferred_element_type=jnp.float32
            )
            amplitude = halves(jnp.concatenate(modal, axis=0) / (1.0 + rates))
            inverse = 1.0 / (1.0 + diff_ref[1] * square)
            mine = dot3(own, amplitude, ((1,), (0,))) * inverse
            for c in range(parts):
                put(1, i, c, mine)
            hold_ref[late_block, i] = encode(dot3(other, amplitude, ((1,), (0,))) * inverse, back_octaves, back_top)
        swap(late_block).start()

    @pl.when(step == pl.num_programs(0) - 1)
    def _():
        lax.fori_loop(0, 2 * chunks, lambda at, _: (wait_most(there_ref, here_ref, there_sems.at[0, at], there_at(at), count), 0)[1], 0)
        lax.fori_loop(0, rows - per_chunk, lambda at, _: (wait_most(back_ref, home_ref, back_sems.at[0, at], row_at(at), count), 0)[1], 0)
        lax.fori_loop(rows - per_chunk, rows + per_chunk, lambda at, _: (wait_most(back_ref, home_ref, back_sems.at[0, at], tail_at(at), count), 0)[1], 0)
        lax.fori_loop(0, blocks, lambda at, _: (swap(at).wait(), 0)[1], 0)


def whole_step(state, legendre, lat, diffusion, modes, rates, gain, b1, b2, b3, perm, synthesis, analysis, w1, w2, w3):
    fields, lev_dev, m_dev, parts, degrees = state.shape
    waves, slabs = lax.axis_size("wave"), lax.axis_size("level")
    count, feats, mc = waves * slabs, fields * lev_dev, m_dev * parts
    tile = legendre.shape[1] // (waves * chunks)
    legendre = legendre.reshape(m_dev, waves, chunks, tile, degrees)
    per_chunk = tile // slabs
    rows = chunks * per_chunk
    m_block = 4
    blocks = m_dev // m_block
    first_steps = chunks * blocks
    last = first_steps - 1
    grid_steps = first_steps + rows
    there = (chunks, 2, count, per_chunk, mc // 2, feats)
    back = (rows, count, mc, feats)
    small = (modes, rates, gain, b1, b2, b3, perm)
    large = (synthesis, analysis, w1, w2, w3)
    swap = (blocks, m_block, lev_dev, degrees)
    lined = by_lanes(state)
    line_block = (lined.shape[0], lined.shape[1] // blocks, lanes)
    any_spec = pl.BlockSpec(memory_space=pl.ANY)
    smem = pl.BlockSpec(memory_space=pltpu.SMEM)
    bf16, f32 = jnp.bfloat16, jnp.float32
    pair = lambda i: jnp.where(i < first_steps, i, jnp.maximum(i - grid_steps, 0))
    return pl.pallas_call(
        step_kernel,
        grid=(grid_steps + first_steps,),
        out_shape=(jax.ShapeDtypeStruct(lined.shape, f32), jax.ShapeDtypeStruct(swap, bf16)),
        in_specs=[
            smem,
            smem,
            pl.BlockSpec(line_block, lambda i: (0, jnp.minimum(i, last) % blocks, 0)),
            pl.BlockSpec((m_block, waves, None, tile, degrees), lambda i: (pair(i) % blocks, 0, pair(i) // blocks, 0, 0)),
            *[whole_block(x) for x in small],
            *[any_spec for _ in large],
        ],
        out_specs=(
            pl.BlockSpec(line_block, lambda i: (0, jnp.maximum(i - (grid_steps + first_steps - blocks), 0), 0)),
            any_spec,
        ),
        scratch_shapes=[
            pltpu.VMEM((count * per_chunk * mc, feats), f32),
            pltpu.VMEM(there, bf16),
            pltpu.VMEM(there, bf16),
            pltpu.VMEM(back, bf16),
            pltpu.VMEM(back, bf16),
            pltpu.VMEM((m_dev, parts * feats, degrees), f32),
            pltpu.VMEM(swap, bf16),
            pltpu.VMEM((slabs * feats, slabs * feats), f32),
            pltpu.VMEM(gain.shape, f32),
            pltpu.VMEM(b3.shape, f32),
            *[pltpu.VMEM(x.shape, bf16) for x in large],
            pltpu.SemaphoreType.DMA((2, 2 * chunks)),
            pltpu.SemaphoreType.DMA((2, rows + per_chunk)),
            pltpu.SemaphoreType.DMA((2, blocks)),
            pltpu.SemaphoreType.DMA((len(large),)),
        ],
        compiler_params=remote_params(),
    )(lat, diffusion, lined, legendre, *small, *large)


def merge_kernel(parts, old_ref, got_ref, out_ref):
    per_block, per_lev, _ = out_ref.shape
    blocks, m_block, lev_dev, degrees = got_ref.shape
    tiles = degrees // lanes
    other = 1 - lax.axis_index("level")
    out_ref[...] = old_ref[...]

    @pl.when(pl.program_id(0) == 0)
    def _():
        out_rows = out_ref.reshape(per_block * per_lev, lanes)
        for b in range(blocks):
            for i in range(m_block):
                value = decode(got_ref[b, i], back_octaves, back_top)
                for t in range(tiles):
                    at = lev_dev * per_lev + ((b * m_block + i) * tiles + t) * parts + other
                    out_rows[pl.ds(at, lev_dev, stride=per_lev), :] = value[:, t * lanes : (t + 1) * lanes]


def merge_step(fields, parts, lined, got):
    blocks = fields // 2 if fields % 2 == 0 else 1
    block = pl.BlockSpec((lined.shape[0] // blocks, *lined.shape[1:]), lambda i: (i, 0, 0))
    return pl.pallas_call(
        functools.partial(merge_kernel, parts),
        grid=(blocks,),
        out_shape=jax.ShapeDtypeStruct(lined.shape, jnp.float32),
        in_specs=[block, whole_block(got)],
        out_specs=block,
    )(lined, got)


def fast_body(longitudes, state, legendre, lat_weight, modes, mode_rates, diffusion, norm_gain, w_first, b_first, w_second, b_second, w_third, b_third):
    fields, lev_dev, m_dev, parts, degrees = state.shape
    levels = modes.shape[0]
    wave_count, level_count = lax.axis_size("wave"), lax.axis_size("level")
    synthesis, analysis = fourier_tables(degrees, longitudes, wave_count, 1.0)
    place = np.arange(fields * levels).reshape(fields, level_count, lev_dev).swapaxes(0, 1).reshape(-1)
    perm = np.zeros((fields * levels, fields * levels), jnp.bfloat16)
    perm[place, np.arange(fields * levels)] = 1.0
    out, got = whole_step(
        state,
        legendre,
        lat_weight,
        diffusion,
        modes,
        mode_rates[None],
        norm_gain[None],
        b_first[None],
        b_second[None],
        b_third[None],
        perm,
        synthesis,
        analysis,
        w_first,
        w_second,
        w_third,
    )
    return from_lanes(merge_step(fields, parts, out, got), state.shape)


def solution(mesh):
    wave_count, level_count = mesh.shape["wave"], mesh.shape["level"]

    def step(state, legendre, *rest):
        longitudes = 2 * legendre.shape[1]
        fields, levels, waves, _, degrees = state.shape
        fits = (
            level_count == 2
            and waves % (16 * wave_count) == 0
            and fields * levels % (128 * level_count) == 0
            and levels % (8 * level_count) == 0
            and legendre.shape[1] % (8 * chunks * wave_count) == 0
            and degrees % 128 == 0
        )
        mapped = jax.shard_map(
            functools.partial(fast_body if fits else general_body, longitudes),
            mesh=mesh,
            in_specs=(P(None, "level", "wave", None, None), P("wave", None, None), P("wave")) + (P(),) * 10,
            out_specs=P(None, "level", "wave", None, None),
            check_vma=False,
        )
        return mapped(state, legendre, *rest)

    return step
```
